32 devices in a mesh: tm: 8 (over y, x, core), space: 4 (over z).
Axes of the slice: x: 2, y: 2, z: 4, core: 2. Of those that a mesh axis runs over, the one named last changes fastest.
Arguments:
- speed: float32 [8, 16, 128], P('space'), may hold values from 0.5 to 1.5
- forcing: float32 [32, 8, 16, 128], P('tm', 'space'), may hold values from -1.8 to 1.8
- guess: float32 [8, 4, 8, 16, 128], P('tm', None, 'space'), may hold values from -8 to 8
- basis: float32 [8, 64, 4, 8, 16, 128], P('tm', None, None, 'space'), may hold values from -1 to 1, as said below
Outputs:
- states: float32 [32, 4, 8, 16, 128], P('tm', None, 'space')
- coords: float32 [8, 64], P('tm')
The draws below stay inside these ranges and needn't reach their ends.
Inputs may be any that keep to these rules, and one draw needn't show every extreme that they name: The columns of each basis[k] are linearly independent.
All inputs are finite; a program needn't handle non-finite values.
Results may differ from the reference program's by a relative error of at most 0.00018.
Values sent between devices are 32-bit elements; how exact they have to be, the bound alone decides.
A program may use at most 128 MiB of HBM per device.

```python
import jax
import jax.numpy as jnp
from jax import lax

NX = 16
NY = 128
RANK = 64
NZ = 8
NT = 32
N_TM = 8


DT = 0.045


def shifted_ahead_drawn(values, axis):
    size = values.shape[axis]
    rest = lax.slice_in_dim(values, 1, size, axis=axis)
    border = jnp.zeros_like(lax.slice_in_dim(values, 0, 1, axis=axis))
    return jnp.concatenate([rest, border], axis=axis)


def shifted_behind_drawn(values, axis):
    size = values.shape[axis]
    rest = lax.slice_in_dim(values, 0, size - 1, axis=axis)
    border = jnp.zeros_like(lax.slice_in_dim(values, 0, 1, axis=axis))
    return jnp.concatenate([border, rest], axis=axis)


def fine_advance(state, speed_sq):
    pressure = state[..., 0, :, :, :]
    depth = pressure.ndim
    flow_x = state[..., 1, :, :, :] - DT * (shifted_ahead_drawn(pressure, depth - 2) - pressure)
    flow_y = state[..., 2, :, :, :] - DT * (shifted_ahead_drawn(pressure, depth - 1) - pressure)
    flow_z = state[..., 3, :, :, :] - DT * (shifted_ahead_drawn(pressure, depth - 3) - pressure)
    diverge = flow_x - shifted_behind_drawn(flow_x, depth - 2) + (flow_y - shifted_behind_drawn(flow_y, depth - 1)) + (flow_z - shifted_behind_drawn(flow_z, depth - 3))
    fresh = pressure - DT * speed_sq * diverge
    return jnp.stack([fresh, flow_x, flow_y, flow_z], axis=depth - 3)


def speed_field(key):
    log_speed = jax.random.uniform(jax.random.fold_in(key, 202), (NZ, NX, NY), jnp.float32, jnp.log(0.5), jnp.log(1.5))
    return jnp.clip(jnp.exp(log_speed), 0.5, 1.5)


def pattern_block(key, block_index):
    return jax.random.normal(jax.random.fold_in(jax.random.fold_in(key, 101), block_index), (RANK, 4, NZ, NX, NY), jnp.float32)


def draw_speed(key, part):
    return speed_field(key)


def draw_guess(key, part):
    mixing = jax.random.normal(jax.random.fold_in(key, 404), (N_TM, RANK), jnp.float32)

    def aligned(block_index):
        block = pattern_block(key, block_index)
        factors = mixing[block_index][:, None, None, None, None]
        return jnp.sum(factors * block, axis=0) / jnp.sqrt(jnp.float32(RANK))
    aligned_all = lax.map(aligned, jnp.arange(N_TM, dtype=jnp.int32))
    rough_part = jax.random.normal(jax.random.fold_in(key, 303), aligned_all.shape, jnp.float32)
    strength = 1.0
    return jnp.clip(rough_part + strength * aligned_all, -8.0, 8.0)


def draw_basis(key, part):
    speed_sq = jnp.square(speed_field(key))
    cell_count = 4 * NZ * NX * NY
    blend_weight = 0.0
    least_scale = 0.3
    most_scale = 3.0
    scales = jnp.exp(jax.random.uniform(jax.random.fold_in(key, 505), (N_TM, RANK), jnp.float32, jnp.log(least_scale), jnp.log(most_scale)))

    def column_block(block_index):
        source = (block_index + N_TM - 2) % N_TM
        moved_block = pattern_block(key, source)
        for repeat in range(4):
            moved_block = fine_advance(moved_block, speed_sq)
        common = jnp.sum(moved_block, axis=0) / jnp.sqrt(jnp.float32(RANK))
        mixed_columns = moved_block + blend_weight * common[None]
        column_scale = scales[block_index] / jnp.sqrt(jnp.float32(cell_count))
        return mixed_columns * column_scale[:, None, None, None, None]
    columns = lax.map(column_block, jnp.arange(N_TM, dtype=jnp.int32))
    return jnp.clip(columns, -1.0, 1.0)


def steps_of(own_key, extent, cuts, least, largest):
    level = 1.0
    for axis_at, shards_of in cuts:
        draws = jax.random.uniform(jax.random.fold_in(jax.random.fold_in(own_key, 6), axis_at), (shards_of,), jnp.float32, least / len(cuts), largest / len(cuts))
        level = level * jnp.repeat(jnp.exp(draws), extent[axis_at] // shards_of).reshape((-1,) + (1,) * (len(extent) - 1 - axis_at))
    return level


def bell_draw(own_key, shape, scale, most, cuts=(), held_as=jnp.bfloat16):
    drawn = scale * jax.random.normal(own_key, shape, jnp.float32)
    if cuts:
        drawn = drawn * steps_of(own_key, shape, cuts, -0.22, 0.18)
    return jnp.clip(drawn, -most, most).astype(held_as)


def setup_inputs(seed: int = 0) -> dict:
    key_list = jax.random.split(jax.random.key(seed), 5)
    return {
        "speed": draw_speed(jax.random.fold_in(key_list[4], 71), 0),
        "forcing": bell_draw(key_list[1], (NT, NZ, NX, NY), 0.3, 1.8, ((0, 8), (1, 4)), jnp.float32),
        "guess": draw_guess(jax.random.fold_in(key_list[4], 71), 0),
        "basis": draw_basis(jax.random.fold_in(key_list[4], 71), 0),
    }


DT = 0.045
exact_mode = lax.Precision.HIGHEST

def shifted_ahead(values, axis):
    size = values.shape[axis]
    rest = lax.slice_in_dim(values, 1, size, axis=axis)
    border = jnp.zeros_like(lax.slice_in_dim(values, 0, 1, axis=axis))
    return jnp.concatenate([rest, border], axis=axis)

def shifted_behind(values, axis):
    size = values.shape[axis]
    rest = lax.slice_in_dim(values, 0, size - 1, axis=axis)
    border = jnp.zeros_like(lax.slice_in_dim(values, 0, 1, axis=axis))
    return jnp.concatenate([border, rest], axis=axis)

def update_flow(state, upper_plane, delta_time):
    pressure = state[..., 0, :, :, :]
    depth = pressure.ndim
    above = jnp.concatenate([pressure[..., 1:, :, :], upper_plane], axis=depth - 3)
    flow_x = state[..., 1, :, :, :] - delta_time * (shifted_ahead(pressure, depth - 2) - pressure)
    flow_y = state[..., 2, :, :, :] - delta_time * (shifted_ahead(pressure, depth - 1) - pressure)
    flow_z = state[..., 3, :, :, :] - delta_time * (above - pressure)
    return (pressure, flow_x, flow_y, flow_z)

def update_pressure(pressure, flow_x, flow_y, flow_z, lower_plane, speed_sq, delta_time):
    depth = pressure.ndim
    below = jnp.concatenate([lower_plane, flow_z[..., :-1, :, :]], axis=depth - 3)
    diverge = flow_x - shifted_behind(flow_x, depth - 2) + (flow_y - shifted_behind(flow_y, depth - 1)) + (flow_z - below)
    fresh = pressure - delta_time * speed_sq * diverge
    return jnp.stack([fresh, flow_x, flow_y, flow_z], axis=depth - 3)

def advance(state, speed_sq, delta_time):
    zero_plane = jnp.zeros_like(state[..., 0, :1, :, :])
    pressure, flow_x, flow_y, flow_z = update_flow(state, zero_plane, delta_time)
    return update_pressure(pressure, flow_x, flow_y, flow_z, zero_plane, speed_sq, delta_time)

def solve_gram(chol, coef):
    lifted = lax.linalg.triangular_solve(chol, coef[..., None], left_side=True, lower=True)
    solved = lax.linalg.triangular_solve(chol, lifted, left_side=True, lower=True, transpose_a=True)
    return solved[..., 0]

def reference(speed, forcing, guess, basis):
    count = guess.shape[0]
    speed_sq = speed * speed
    loads = forcing.reshape(count, 4, forcing.shape[1], forcing.shape[2], forcing.shape[3])

    def fine_step(state, row_index):
        moved = advance(state, speed_sq, DT)
        return moved.at[:, 0].add(loads[:, row_index])

    def sweep(left):
        points = []
        current = left
        for row_index in range(3):
            current = fine_step(current, row_index)
            points.append(current)
        return points

    def from_left(values):
        return jnp.roll(values, 1, axis=0)
    first_points = sweep(from_left(guess))
    relaxed = fine_step(first_points[-1], 3)
    second_points = sweep(from_left(relaxed))
    residue = fine_step(second_points[-1], 3) - relaxed
    flat_basis = basis.reshape(count, basis.shape[1], -1)

    def build(columns):
        moved = columns
        for repeat in range(4):
            moved = advance(moved, speed_sq, DT)
        return (moved - advance(columns, speed_sq, 4 * DT)).reshape(columns.shape[0], -1)
    corrections = lax.map(build, basis)
    gram = jnp.einsum('krn,ksn->krs', flat_basis, flat_basis, precision=exact_mode)
    chol = jnp.linalg.cholesky(gram)

    def candidate(levels):
        left = from_left(levels)
        moved = advance(left, speed_sq, 4 * DT)
        coef = jnp.einsum('krn,kn->kr', flat_basis, left.reshape(count, -1), precision=exact_mode)
        weights = solve_gram(chol, coef)
        extra = jnp.einsum('kr,krn->kn', weights, corrections, precision=exact_mode).reshape(left.shape)
        return moved + extra + residue
    levels = candidate(residue)
    levels = candidate(levels)
    gap = candidate(levels) - levels
    carry = gap[0:4]
    chained = [carry]
    for group in range(1, count // 4):
        carry = advance(advance(carry, speed_sq, 8 * DT), speed_sq, 8 * DT) + gap[4 * group:4 * group + 4]
        chained.append(carry)
    chain = jnp.concatenate(chained, axis=0)
    levels = candidate(levels + chain)
    final_c = relaxed + levels
    third_points = sweep(from_left(final_c))
    states = jnp.stack(third_points + [final_c], axis=1)
    states = states.reshape(count * 4, 4, guess.shape[2], guess.shape[3], guess.shape[4])
    coef = jnp.einsum('krn,kn->kr', flat_basis, final_c.reshape(count, -1), precision=exact_mode)
    coords = solve_gram(chol, coef)
    return (states, coords)
```

```python
import jax
import jax.numpy as jnp
from jax import lax
from jax.experimental import pallas as pl
from jax.experimental.pallas import tpu as pltpu
from jax.sharding import PartitionSpec as P

DT = 0.045
GROUP = 4
MESH = pl.DeviceIdType.MESH
VX, VY, VZ, DV, PR = range(5)


def make_kernel(n_tm, n_sp, rank, slab, nx, ny):
    n_chain = n_tm // GROUP - 1
    reach_max = max(4, 2 * n_chain)
    base = reach_max
    own_planes = range(base, base + slab)

    def span(lo, hi, first):
        lo, hi = max(lo, first), min(hi, first + slab)
        return (lo - first, hi - lo) if hi > lo else None

    def pieces(reach, keep):
        made = [] if keep is None else [(0, keep, 5 - keep, 0, slab)]
        far = -(-reach // slab)
        for dist in range(1, far + 1):
            for delta in (dist, -dist):
                first = base - delta * slab
                need = {
                    PR: span(base - reach, base + slab + reach, first),
                    DV: span(base - reach + 1, base + slab + reach - 1, first),
                }
                above = first + slab
                if base - reach + 1 <= above < base + slab + reach - 1:
                    need[VZ] = (slab - 1, 1)
                fields = sorted(need)
                at = 0
                while at < len(fields):
                    end = at + 1
                    while end < len(fields) and need[fields[end]] == need[fields[at]]:
                        end += 1
                    if need[fields[at]] is not None:
                        o, n = need[fields[at]]
                        made.append((delta, fields[at], end - at, o, n))
                    at = end
        return made

    def load_pieces(steps, keep):
        made = [(0, 0, steps, 0, slab)] if keep else []
        far = -(-(steps - 1) // slab)
        for dist in range(1, far + 1):
            for delta in (dist, -dist):
                first = base - delta * slab
                at = 0
                while at < steps - 1:
                    here = span(base - steps + 1 + at, base + slab + steps - 1 - at, first)
                    end = at + 1
                    while end < steps - 1 and here == span(
                        base - steps + 1 + end, base + slab + steps - 1 - end, first
                    ):
                        end += 1
                    if here is not None:
                        made.append((delta, at, end - at, here[0], here[1]))
                    at = end
        return made

    speed_pieces = [(d, 0, 1, o, n) for d, f, m, o, n in pieces(reach_max - 1, None) if f <= PR < f + m]

    def kernel(
        speed_in, forcing_in, guess_in, basis_in, states_out, coords_out,
        gl, fl, basis, cw, c2, fw, fo, wv, win, xs, tb, cf, gb, inv, acc, wb,
        local_sem, send_sems, recv_sems,
    ):
        k = lax.axis_index("tm")
        s = lax.axis_index("space")
        before = lax.rem(k + n_tm - 1, n_tm)

        def block(offset):
            return lax.rem(k + offset + n_tm, n_tm)

        def peer(d):
            return lax.rem(s + d, n_sp)

        def inside(at):
            return (at >= 0) & (at < n_sp)

        own = pl.ds(base, slab)
        copies = [
            pltpu.make_async_copy(guess_in, gl, local_sem.at[0]),
            pltpu.make_async_copy(forcing_in, fl, local_sem.at[1]),
            pltpu.make_async_copy(speed_in, cw.at[:, own], local_sem.at[2]),
            pltpu.make_async_copy(basis_in, basis, local_sem.at[3]),
        ]
        for c in copies:
            c.start()

        wins = {}
        senders = {}

        def name(key, reach):
            wins[key] = (win.at[len(wins)], reach)
            senders[key] = wv.at[len(senders)]

        name("guess", 4)
        name("relaxed", 4)
        for i in range(3):
            name(("x", i), 1)
            name(("y", i), 4)
        for j in range(1, n_chain + 1):
            name(("gap", j), 2 * j)
        name("x3", 1)
        name("y3", 4)
        name("final", 3)

        missing = {}
        for ref, reach in wins.values():
            for piece in pieces(reach, None):
                missing.setdefault(piece[0], []).append((ref, piece))
        for ref, part in ((fw, load_pieces(4, False)), (fo, load_pieces(3, False)), (cw, speed_pieces)):
            for piece in part:
                missing.setdefault(piece[0], []).append((ref, piece))
        for delta, regions in missing.items():
            def clear(regions=regions):
                for ref, (d, f, m, o, n) in regions:
                    at = base - d * slab + o
                    for i in range(f, f + m):
                        ref[i, at:at + n] = jnp.zeros((n, nx, ny), jnp.float32)

            pl.when(jnp.logical_not(inside(s - delta)))(clear)

        offsets = set()
        for off in [1, 2] + [GROUP * j for j in range(1, n_chain + 1)]:
            offsets |= {off % n_tm, -off % n_tm}
        partners = [(k, peer(d)) for d in range(1, n_sp)]
        for off in sorted(offsets - {0}):
            partners += [(block(off), peer(d)) for d in range(n_sp)]
        barrier = pltpu.get_barrier_semaphore()
        for target in partners:
            pl.semaphore_signal(barrier, inc=1, device_id=target, device_id_type=MESH)

        sent = []

        class Remote:
            def __init__(self, src, dst, target, sends=None, receives=None):
                i = len(sent)
                self.copy = pltpu.make_async_remote_copy(
                    src_ref=src, dst_ref=dst, send_sem=send_sems.at[i], recv_sem=recv_sems.at[i],
                    device_id=target, device_id_type=MESH,
                )
                self.sends, self.receives = sends, receives
                sent.append(self)
                self.under(sends, self.copy.start)

            def under(self, condition, act):
                if condition is None:
                    act()
                else:
                    pl.when(condition)(act)

            def wait_recv(self):
                self.under(self.receives, self.copy.wait_recv)

            def wait_send(self):
                self.under(self.sends, self.copy.wait_send)

        def both(a, b):
            return b if a is None else a if b is None else a & b

        def spread(src, at, dst, group, parts, sends=None, receives=None):
            made = []
            for delta, f, m, o, n in parts:
                made.append(Remote(
                    src.at[pl.ds(f, m), pl.ds(at + o, n)],
                    dst.at[pl.ds(f, m), pl.ds(base - delta * slab + o, n)],
                    (group, s + delta),
                    both(sends, None if delta == 0 else inside(s + delta)),
                    both(receives, None if delta == 0 else inside(s - delta)),
                ))
            return made

        def wait(made):
            for c in made:
                c.wait_recv()

        row = lax.broadcasted_iota(jnp.int32, (nx, ny), 0)
        lane = lax.broadcasted_iota(jnp.int32, (nx, ny), 1)
        first_row, last_row = row == 0, row == nx - 1
        first_lane, last_lane = lane == 0, lane == ny - 1

        def ahead(p, axis):
            n, last = ((nx, last_row), (ny, last_lane))[axis]
            return jnp.where(last, 0.0, pltpu.roll(p, n - 1, axis))

        def behind(p, axis, border):
            return jnp.where((first_row, first_lane)[axis], border, pltpu.roll(p, 1, axis))

        def floor(z):
            if z <= base and (base - z) % slab == 0:
                return jnp.where(s > (base - z) // slab, 1.0, 0.0)
            return None

        def lap(p, z):
            c = p[z]
            down = c - p[z - 1]
            edge = floor(z)
            if edge is not None:
                down = down * edge
            flat = (ahead(c, 0) + behind(c, 0, c)) + (ahead(c, 1) + behind(c, 1, c)) - 4.0 * c
            return flat + ((p[z + 1] - c) - down)

        def grad(p, z):
            c = p[z]
            return ahead(c, 0) - c, ahead(c, 1) - c, p[z + 1] - c

        def part_div(vx, vy, vz, z):
            d = (vx[z] - behind(vx[z], 0, 0.0)) + (vy[z] - behind(vy[z], 1, 0.0))
            return d + (vz[z] if z == base else vz[z] - vz[z - 1])

        def load_window(ref, reach):
            p = {z: ref[PR, z] for z in range(base - reach, base + slab + reach)}
            d = {}
            for z in range(base - reach + 1, base + slab + reach - 1):
                d[z] = ref[DV, z]
                if (z - base) % slab == 0:
                    d[z] = d[z] - ref[VZ, z - 1]
            return p, d

        def load_flow(ref):
            return tuple({z: ref[f, z] for z in own_planes} for f in (VX, VY, VZ))

        def store_state(ref, at, p, v):
            for z in own_planes:
                for f in (VX, VY, VZ):
                    ref[f, z - base + at] = v[f][z]
                ref[DV, z - base + at] = part_div(*v, z)
                ref[PR, z - base + at] = p[z]

        def scale(z, h):
            return h * c2[z]

        def evolve(p, d, steps, h, loads=None):
            total = None
            for i in range(steps):
                reach = steps - 1 - i
                kept = {z: p[z] for z in range(base, base + slab + 1)}
                total = kept if total is None else {z: total[z] + kept[z] for z in kept}
                fresh, nd = {}, {}
                for z in range(base - reach, base + slab + reach):
                    nd[z] = d[z] - h * lap(p, z)
                    fresh[z] = p[z] - scale(z, h) * nd[z]
                    if loads is not None:
                        fresh[z] = fresh[z] + loads(i, z)
                p, d = fresh, nd
            return p, d, total

        def push(v, total, h):
            out = ({}, {}, {})
            for z in own_planes:
                g = grad(total, z)
                for f in range(3):
                    out[f][z] = v[f][z] - h * g[f]
            return out

        def send(key, group, reach, keep, sends=None, receives=None):
            return spread(senders[key], 0, wins[key][0], group, pieces(reach, keep), sends, receives)

        copies[0].wait()
        p = {z: gl[0, z - base] for z in own_planes}
        v = tuple({z: gl[1 + f, z - base] for z in own_planes} for f in range(3))
        store_state(senders["guess"], 0, p, v)
        copies[1].wait()
        copies[2].wait()
        pl.semaphore_wait(barrier, len(partners))

        first = send("guess", block(2), 4, VX)
        first += spread(fl, 0, fw, block(1), load_pieces(4, True))
        first += spread(cw, base, cw, k, speed_pieces)

        copies[3].wait()

        def gram_step(i, total):
            t = jnp.swapaxes(basis[:, i], 0, 1)
            hi = t.astype(jnp.bfloat16)
            rest = t - hi.astype(jnp.float32)
            mid = rest.astype(jnp.bfloat16)
            low = (rest - mid.astype(jnp.float32)).astype(jnp.bfloat16)
            parts = jnp.concatenate([hi, mid, low], axis=1)
            flat = jnp.concatenate([parts[j] for j in range(parts.shape[0])], axis=1)
            return total + lax.dot_general(
                flat, flat, (((1,), (1,)), ((), ())), preferred_element_type=jnp.float32
            )

        full = lax.fori_loop(0, basis.shape[1], gram_step, jnp.zeros((3 * rank, 3 * rank), jnp.float32))
        hh, hm, hl = full[:rank, :rank], full[:rank, rank:2 * rank], full[:rank, 2 * rank:]
        mh, mm, lh = full[rank:2 * rank, :rank], full[rank:2 * rank, rank:2 * rank], full[2 * rank:, :rank]
        gram = hh + ((hm + mh) + (mm + (hl + lh)))
        gb[s] = jnp.concatenate([gram[:rank // 2], gram[rank // 2:]], axis=1)

        wait(first)
        for z in range(1, 2 * base + slab - 1):
            c2[z] = cw[0, z] * cw[0, z]

        def loads(i, z):
            return fw[i, z]

        p, d = load_window(wins["guess"][0], 4)
        p, d, total = evolve(p, d, 4, DT, loads)
        v = push(load_flow(wins["guess"][0]), total, DT)
        store_state(senders["relaxed"], 0, p, v)
        moved = send("relaxed", block(1), 4, VX)
        gram_copies = [Remote(gb.at[s], gb.at[s], (k, peer(d))) for d in range(1, n_sp)]
        late_loads = spread(fl, 0, fo, k, load_pieces(3, False))

        def dot(index, p, v):
            for z in own_planes:
                xs[z - base] = p[z]
                for f in range(3):
                    xs[(1 + f) * slab + z - base] = v[f][z]
            x = xs[...]

            def coef_step(i, carry):
                b = basis[pl.ds(8 * i, 8)]
                t = jnp.sum(b * x[None], axis=1)
                half = t.shape[1] // 2
                t = t[:, :half] + t[:, half:]
                acc[pl.ds(pl.multiple_of(8 * i, 8), 8), :] = jnp.sum(t, axis=1)
                return carry

            lax.fori_loop(0, rank // 8, coef_step, 0)
            ones = jnp.ones((8, acc.shape[1]), jnp.float32)
            cf[index, s] = lax.dot_general(
                ones, acc[...], (((1,), (1,)), ((), ())),
                precision=lax.Precision.HIGHEST, preferred_element_type=jnp.float32,
            )
            line = pl.ds(0, 1)
            return [
                Remote(cf.at[index, s, line], cf.at[index, s, line], (k, peer(d)))
                for d in range(1, n_sp)
            ]

        def solve(index, made):
            wait(made)
            total = cf[index, 0, 0:1]
            for i in range(1, n_sp):
                total = total + cf[index, i, 0:1]
            w = jnp.sum(inv[...] * total, axis=1, keepdims=True)
            return jnp.broadcast_to(w, wb.shape)

        def combine(index, made):
            wb[...] = solve(index, made)

            def sum_step(r, y):
                return y + wb[pl.ds(r, 1), :][None] * basis[r]

            y = lax.fori_loop(0, rank, sum_step, jnp.zeros(basis.shape[1:], jnp.float32), unroll=4)
            return [{z: y[f * slab + z - base] for z in own_planes} for f in range(4)]

        def store_y(ref, at, y):
            for z in own_planes:
                ref[VZ, z - base + at] = y[3][z]
                ref[DV, z - base + at] = part_div(*y[1:], z)
                ref[PR, z - base + at] = y[0][z]

        def coarse(ref):
            p, d = load_window(ref, 1)
            h = 4 * DT
            out = {z: p[z] - scale(z, h) * (d[z] - h * lap(p, z)) for z in own_planes}
            return out, push(load_flow(ref), {z: p[z] for z in range(base, base + slab + 1)}, h)

        def corrected(ref, p, v):
            q, d = load_window(ref, 4)
            h = 4 * DT
            late, _, total = evolve(q, d, 4, DT)
            change = {z: total[z] - 4.0 * q[z] for z in range(base, base + slab + 1)}
            out = {}
            for z in own_planes:
                out[z] = p[z] + (late[z] - (q[z] - scale(z, h) * (d[z] - h * lap(q, z))))
            return out, push(v, change, DT)

        wait(moved)
        p, d = load_window(wins["relaxed"][0], 4)
        p, d, total = evolve(p, d, 4, DT, loads)
        v = push(load_flow(wins["relaxed"][0]), total, DT)
        for z in own_planes:
            tb[0, 3, z - base] = p[z]
            for f in (VX, VY, VZ):
                tb[0, f, z - base] = v[f][z]
        rel = senders["relaxed"]
        p = {z: p[z] - rel[PR, z - base] for z in own_planes}
        v = tuple({z: v[f][z] - rel[f, z - base] for z in own_planes} for f in range(3))
        made = dot(0, p, v)
        store_state(senders[("x", 0)], 0, p, v)
        x_moved = send(("x", 0), block(1), 1, VX)

        wait(gram_copies)
        g = gb[0]
        for i in range(1, n_sp):
            g = g + gb[i]
        g = jnp.concatenate([g, pltpu.roll(g, rank, 1)], axis=0)
        rows = lax.broadcasted_iota(jnp.int32, g.shape, 0)
        lanes = lax.broadcasted_iota(jnp.int32, g.shape, 1)
        m = jnp.where(lanes < rank, g, jnp.where(lanes == rows + rank, 1.0, 0.0))
        for j in range(rank):
            pivot = m[j:j + 1]
            pivot = pivot / pivot[:, j:j + 1]
            m = jnp.where(rows == j, pivot, m - m[:, j:j + 1] * pivot)
        inverse = m[:, rank:]
        inv[...] = jnp.concatenate([inverse, jnp.zeros_like(inverse)], axis=1)

        res = senders[("x", 0)]
        back = []
        for i in range(3):
            y = combine(i, made)
            store_y(senders[("y", i)], 0, y)
            y_moved = send(("y", i), block(1), 4, VZ)
            if i == 0:

                back = [Remote(tb.at[0], tb.at[1], (before, s))]
            wait(x_moved)
            p, v = coarse(wins[("x", i)][0])
            p = {z: p[z] + res[PR, z - base] for z in own_planes}
            v = tuple({z: v[f][z] + res[f, z - base] for z in own_planes} for f in range(3))
            wait(y_moved)
            p, v = corrected(wins[("y", i)][0], p, v)
            if i < 2:
                made = dot(i + 1, p, v)
                store_state(senders[("x", i + 1)], 0, p, v)
                x_moved = send(("x", i + 1), block(1), 1, VX)

        old = senders[("x", 2)]
        gap_p = {z: p[z] - old[PR, z - base] for z in own_planes}
        gap_v = tuple({z: v[f][z] - old[f, z - base] for z in own_planes} for f in range(3))
        chains = []
        for j in range(1, n_chain + 1):
            if j == 1:
                store_state(senders[("gap", 1)], 0, gap_p, gap_v)
            chains.append(spread(
                senders[("gap", 1)], 0, wins[("gap", j)][0], block(GROUP * j), pieces(2 * j, VX),
                before + GROUP * j < n_tm, before >= GROUP * j,
            ))
        carry = None
        for j in range(n_chain, 0, -1):
            wait(chains[j - 1])
            ref = wins[("gap", j)][0]
            used = before >= GROUP * j
            q, d = load_window(ref, 2 * j)
            u = load_flow(ref)

            def kept(planes):
                return {z: jnp.where(used, planes[z], 0.0) for z in planes}

            q, d, u = kept(q), kept(d), tuple(kept(a) for a in u)
            if carry is not None:
                q = {z: q[z] + carry[0][z] for z in q}
                d = {z: d[z] + carry[1][z] for z in d}
                u = tuple({z: u[f][z] + carry[2][f][z] for z in own_planes} for f in range(3))
            for step in range(2):
                reach = 2 * j - 1 - step
                u = push(u, q, 8 * DT)
                nq, nd = {}, {}
                for z in range(base - reach, base + slab + reach):
                    nd[z] = d[z] - 8 * DT * lap(q, z)
                    nq[z] = q[z] - scale(z, 8 * DT) * nd[z]
                q, d = nq, nd
            carry = (q, d, u)
        if carry is not None:
            p = {z: p[z] + carry[0][z] for z in own_planes}
            v = tuple({z: v[f][z] + carry[2][f][z] for z in own_planes} for f in range(3))
        made = dot(3, p, v)
        ref = wins["x3"][0]
        store_state(ref, base, p, v)
        x_moved = spread(ref, base, ref, k, pieces(1, None))
        wait(x_moved)
        wait(back)
        p, v = coarse(ref)
        p = {z: p[z] + tb[1, 3, z - base] for z in own_planes}
        v = tuple({z: v[f][z] + tb[1, f, z - base] for z in own_planes} for f in range(3))
        y = combine(3, made)
        ref = wins["y3"][0]
        store_y(ref, base, y)
        y_moved = spread(ref, base, ref, k, pieces(4, None))
        wait(y_moved)
        p, v = corrected(ref, p, v)
        store_state(senders["final"], 0, p, v)
        moved = send("final", block(1), 3, VX)
        made = dot(4, p, v)
        for z in own_planes:
            states_out[3, 0, z - base] = p[z]
            for f in range(3):
                states_out[3, 1 + f, z - base] = v[f][z]
        w = solve(4, made)
        rows = lax.broadcasted_iota(jnp.int32, w.shape, 0)
        lanes = lax.broadcasted_iota(jnp.int32, w.shape, 1)
        coords_out[...] = jnp.sum(jnp.where(rows == lanes, w, 0.0), axis=0, keepdims=True)[:, :rank]
        wait(late_loads)
        wait(moved)
        p, d = load_window(wins["final"][0], 3)
        v = load_flow(wins["final"][0])
        for n in range(3):
            reach = 2 - n
            v = push(v, p, DT)
            fresh, nd = {}, {}
            for z in range(base - reach, base + slab + reach):
                nd[z] = d[z] - DT * lap(p, z)
                source = fl[n, z - base] if z in own_planes else fo[n, z]
                fresh[z] = (p[z] - scale(z, DT) * nd[z]) + source
            p, d = fresh, nd
            for z in own_planes:
                states_out[n, 0, z - base] = p[z]
                for f in range(3):
                    states_out[n, 1 + f, z - base] = v[f][z]
        for c in sent:
            c.wait_send()

    n_wins = 2 + 6 + n_chain + 3
    n_sent = (
        len(pieces(4, VX)) * 6 + len(pieces(3, VX)) * 2 + len(pieces(1, VX)) * 4
        + sum(len(pieces(2 * j, VX)) for j in range(1, n_chain + 1))
        + len(load_pieces(4, True)) + len(load_pieces(3, False)) + len(speed_pieces) + 6 * (n_sp - 1) + 1
    )
    return kernel, reach_max, n_wins, n_sent


def solution(mesh):
    n_tm, n_sp = mesh.shape["tm"], mesh.shape["space"]

    def body(speed, forcing, guess, basis):
        rank = basis.shape[1]
        slab, nx, ny = speed.shape
        f32 = jnp.float32
        dma = pltpu.SemaphoreType.DMA
        kernel, reach, n_wins, n_sent = make_kernel(n_tm, n_sp, rank, slab, nx, ny)
        wide = slab + 2 * reach
        return pl.pallas_call(
            kernel,
            out_shape=(
                jax.ShapeDtypeStruct((4, 4, slab, nx, ny), f32),
                jax.ShapeDtypeStruct((1, rank), f32),
            ),
            in_specs=[pl.BlockSpec(memory_space=pl.ANY)] * 4,
            out_specs=(pl.BlockSpec(memory_space=pltpu.VMEM),) * 2,
            scratch_shapes=[
                pltpu.VMEM((4, slab, nx, ny), f32),
                pltpu.VMEM((4, slab, nx, ny), f32),
                pltpu.VMEM((rank, 4 * slab, nx, ny), f32),
                pltpu.VMEM((1, wide, nx, ny), f32),
                pltpu.VMEM((wide, nx, ny), f32),
                pltpu.VMEM((4, wide, nx, ny), f32),
                pltpu.VMEM((3, wide, nx, ny), f32),
                pltpu.VMEM((n_wins, 5, slab, nx, ny), f32),
                pltpu.VMEM((n_wins, 5, wide, nx, ny), f32),
                pltpu.VMEM((4 * slab, nx, ny), f32),
                pltpu.VMEM((2, 4, slab, nx, ny), f32),
                pltpu.VMEM((5, n_sp, 8, 2 * rank), f32),
                pltpu.VMEM((n_sp, rank // 2, 2 * rank), f32),
                pltpu.VMEM((rank, 2 * rank), f32),
                pltpu.VMEM((2 * rank, ny), f32),
                pltpu.VMEM((rank, ny), f32),
                dma((4,)),
                dma((n_sent,)), dma((n_sent,)),
            ],
            compiler_params=pltpu.CompilerParams(
                collective_id=0, has_side_effects=True, vmem_limit_bytes=60 * 1024 * 1024
            ),
        )(speed[None], forcing, guess[0], basis[0].reshape(rank, 4 * slab, nx, ny))

    placed = (
        P("space", None, None),
        P("tm", "space", None, None),
        P("tm", None, "space", None, None),
        P("tm", None, None, "space", None, None),
    )
    return jax.shard_map(
        body,
        mesh=mesh,
        in_specs=placed,
        out_specs=(P("tm", None, "space", None, None), P("tm", None)),
        check_vma=False,
    )
```

```python
import jax
import jax.numpy as jnp
from jax import lax
from jax.experimental import pallas as pl
from jax.experimental.pallas import tpu as pltpu
from jax.sharding import PartitionSpec as P

DT = 0.045
GROUP = 4
MESH = pl.DeviceIdType.MESH
VX, VY, VZ, DV, PR = range(5)


def make_kernel(n_tm, n_sp, rank, slab, nx, ny):
    n_chain = n_tm // GROUP - 1
    reach_max = max(4, 2 * n_chain)
    base = reach_max
    own_planes = range(base, base + slab)

    def span(lo, hi, first):
        lo, hi = max(lo, first), min(hi, first + slab)
        return (lo - first, hi - lo) if hi > lo else None

    def pieces(reach, here, patch):
        made = []
        far = -(-reach // slab)
        for dist in range(far, 0, -1):
            for delta in (dist, -dist):
                first = base - delta * slab
                need = {
                    PR: span(base - reach, base + slab + reach, first),
                    DV: span(base - reach + 1, base + slab + reach - 1, first),
                }
                above = first + slab
                if patch and base - reach + 1 <= above < base + slab + reach - 1:
                    need[VZ] = (slab - 1, 1)
                fields = sorted(need)
                at = 0
                while at < len(fields):
                    end = at + 1
                    while end < len(fields) and need[fields[end]] == need[fields[at]]:
                        end += 1
                    if need[fields[at]] is not None:
                        o, n = need[fields[at]]
                        made.append((delta, fields[at], end - at, o, n))
                    at = end
        if here:
            made.append((0, DV, 2, 0, slab))
            if patch and reach > 1:
                made.append((0, VZ, 1, slab - 1, 1))
        return made

    flow = [(0, VX, 3, 0, slab)]
    rest = [(0, VX, 2, 0, slab)] + ([(0, VZ, 1, 0, slab - 1)] if slab > 1 else [])

    def load_pieces(steps, keep):
        made = []
        far = -(-(steps - 1) // slab)
        for dist in range(far, 0, -1):
            for delta in (dist, -dist):
                first = base - delta * slab
                at = 0
                while at < steps - 1:
                    here = span(base - steps + 1 + at, base + slab + steps - 1 - at, first)
                    end = at + 1
                    while end < steps - 1 and here == span(
                        base - steps + 1 + end, base + slab + steps - 1 - end, first
                    ):
                        end += 1
                    if here is not None:
                        made.append((delta, at, end - at, here[0], here[1]))
                    at = end
        if keep:
            made.append((0, 0, steps, 0, slab))
        return made

    speed_pieces = [(d, 0, 1, o, n) for d, f, m, o, n in pieces(reach_max - 1, False, False) if f <= PR < f + m]

    def kernel(
        speed_in, forcing_in, guess_in, basis_in, states_out, coords_out,
        gl, fl, basis, slim, cw, c2, fw, fo, wv, win, xs, tb, cf, gb, inv, acc, wb,
        local_sem, send_sems, recv_sems,
    ):
        k = lax.axis_index("tm")
        s = lax.axis_index("space")
        before = lax.rem(k + n_tm - 1, n_tm)

        def block(offset):
            return lax.rem(k + offset % n_tm, n_tm)

        def peer(d):
            return lax.rem(s + d, n_sp)

        def inside(at):
            return (at >= 0) & (at < n_sp)


        barrier = pltpu.get_barrier_semaphore()

        def greet(group, at, condition):
            def act():
                pl.semaphore_signal(barrier, inc=1, device_id=(group, at), device_id_type=MESH)

            if condition is None:
                act()
            else:
                pl.when(condition)(act)

        def deltas(reach):
            return sorted({piece[0] for piece in pieces(reach, True, False)}, key=abs)[::-1]

        def one(condition):
            return jnp.where(condition, 1, 0)

        greetings = n_sp
        for off, reach in [(1, 4), (2, 4)]:
            for delta in deltas(reach):
                greet(block(-off), s - delta, None if delta == 0 else inside(s - delta))
                greetings += 1 if delta == 0 else one(inside(s + delta))
        for d in range(n_sp - 1, 0, -1):
            greet(k, peer(d), None)
        for j in range(1, n_chain + 1):
            for delta in deltas(2 * j):
                greet(block(-GROUP * j), s - delta, (before >= GROUP * j) & inside(s - delta))
                greetings += one((before + GROUP * j < n_tm) & inside(s + delta))
        greet(block(1), s, None)

        own = pl.ds(base, slab)
        copies = [
            pltpu.make_async_copy(guess_in, gl, local_sem.at[0]),
            pltpu.make_async_copy(forcing_in, fl, local_sem.at[1]),
            pltpu.make_async_copy(speed_in, cw.at[:, own], local_sem.at[2]),
            pltpu.make_async_copy(basis_in, basis, local_sem.at[3]),
        ]
        for c in copies:
            c.start()

        wins = {}
        senders = {}

        def name(key, reach):
            wins[key] = (win.at[len(wins)], reach)
            senders[key] = wv.at[len(senders)]

        patched = ("guess", "y")
        name(("guess", 0), 4)
        name(("relaxed", 0), 4)
        for i in range(3):
            name(("x", i), 1)
            name(("y", i), 4)
        for j in range(1, n_chain + 1):
            name(("gap", j), 2 * j)
        name(("x", 3), 1)
        name(("y", 3), 4)
        name(("final", 0), 3)

        missing = {}
        for key, (ref, reach) in wins.items():
            for piece in pieces(reach, False, key[0] in patched):
                missing.setdefault(piece[0], []).append((ref, piece))
        for ref, part in ((fw, load_pieces(4, False)), (fo, load_pieces(3, False)), (cw, speed_pieces)):
            for piece in part:
                missing.setdefault(piece[0], []).append((ref, piece))
        for delta, regions in missing.items():
            def clear(regions=regions):
                for ref, (d, f, m, o, n) in regions:
                    at = base - d * slab + o
                    for i in range(f, f + m):
                        ref[i, at:at + n] = jnp.zeros((n, nx, ny), jnp.float32)

            pl.when(jnp.logical_not(inside(s - delta)))(clear)

        sent = []

        class Remote:
            def __init__(self, src, dst, target, sends=None, receives=None):
                i = len(sent)
                self.copy = pltpu.make_async_remote_copy(
                    src_ref=src, dst_ref=dst, send_sem=send_sems.at[i], recv_sem=recv_sems.at[i],
                    device_id=target, device_id_type=MESH,
                )
                self.sends, self.receives = sends, receives
                sent.append(self)
                self.under(sends, self.copy.start)

            def under(self, condition, act):
                if condition is None:
                    act()
                else:
                    pl.when(condition)(act)

            def wait_recv(self):
                self.under(self.receives, self.copy.wait_recv)

            def wait_send(self):
                self.under(self.sends, self.copy.wait_send)

        def both(a, b):
            return b if a is None else a if b is None else a & b

        def spread(src, at, dst, group, parts, sends=None, receives=None):
            made = []
            for delta, f, m, o, n in parts:
                made.append(Remote(
                    src.at[pl.ds(f, m), pl.ds(at + o, n)],
                    dst.at[pl.ds(f, m), pl.ds(base - delta * slab + o, n)],
                    (group, s + delta),
                    both(sends, None if delta == 0 else inside(s + delta)),
                    both(receives, None if delta == 0 else inside(s - delta)),
                ))
            return made

        def wait(made):
            for c in made:
                c.wait_recv()

        row = lax.broadcasted_iota(jnp.int32, (nx, ny), 0)
        lane = lax.broadcasted_iota(jnp.int32, (nx, ny), 1)
        first_row, last_row = row == 0, row == nx - 1
        first_lane, last_lane = lane == 0, lane == ny - 1

        def ahead(p, axis):
            n, last = ((nx, last_row), (ny, last_lane))[axis]
            return jnp.where(last, 0.0, pltpu.roll(p, n - 1, axis))

        def behind(p, axis, border):
            return jnp.where((first_row, first_lane)[axis], border, pltpu.roll(p, 1, axis))

        def floor(z):
            if z <= base and (base - z) % slab == 0:
                return jnp.where(s > (base - z) // slab, 1.0, 0.0)
            return None

        def lap(p, z):
            c = p[z]
            down = c - p[z - 1]
            edge = floor(z)
            if edge is not None:
                down = down * edge
            flat = (ahead(c, 0) + behind(c, 0, c)) + (ahead(c, 1) + behind(c, 1, c)) - 4.0 * c
            return flat + ((p[z + 1] - c) - down)

        def grad(p, z):
            c = p[z]
            return ahead(c, 0) - c, ahead(c, 1) - c, p[z + 1] - c

        def part_div(vx, vy, vz, z):
            d = (vx[z] - behind(vx[z], 0, 0.0)) + (vy[z] - behind(vy[z], 1, 0.0))
            return d + (vz[z] if z == base else vz[z] - vz[z - 1])

        def load_window(ref, reach, patch=False):
            p = {z: ref[PR, z] for z in range(base - reach, base + slab + reach)}
            d = {}
            for z in range(base - reach + 1, base + slab + reach - 1):
                d[z] = ref[DV, z]
                if patch and (z - base) % slab == 0:
                    d[z] = d[z] - ref[VZ, z - 1]
            return p, d

        def load_flow(ref):
            return tuple({z: ref[f, z] for z in own_planes} for f in (VX, VY, VZ))

        def store_wave(ref, p, d):
            for z in own_planes:
                ref[DV, z - base] = d[z]
                ref[PR, z - base] = p[z]

        def store_flow(ref, v):
            for z in own_planes:
                for f in (VX, VY, VZ):
                    ref[f, z - base] = v[f][z]

        def load_state(ref):
            p, d = ({z: ref[f, z - base] for z in own_planes} for f in (PR, DV))
            return p, tuple({z: ref[f, z - base] for z in own_planes} for f in (VX, VY, VZ)), d

        def plus(a, b):
            return {z: a[z] + b[z] for z in own_planes}

        def minus(a, b):
            return {z: a[z] - b[z] for z in own_planes}

        def each(op, a, b):
            return op(a[0], b[0]), tuple(op(x, y) for x, y in zip(a[1], b[1])), op(a[2], b[2])

        def scale(z, h):
            return h * c2[z]

        def evolve(p, d, steps, h, loads=None):
            total = None
            for i in range(steps):
                reach = steps - 1 - i
                kept = {z: p[z] for z in range(base, base + slab + 1)}
                total = kept if total is None else {z: total[z] + kept[z] for z in kept}
                fresh, nd = {}, {}
                for z in range(base - reach, base + slab + reach):
                    nd[z] = d[z] - h * lap(p, z)
                    fresh[z] = p[z] - scale(z, h) * nd[z]
                    if loads is not None:
                        fresh[z] = fresh[z] + loads(i, z)
                p, d = fresh, nd
            return p, d, total

        def push(v, total, h):
            out = ({}, {}, {})
            for z in own_planes:
                g = grad(total, z)
                for f in range(3):
                    out[f][z] = v[f][z] - h * g[f]
            return out

        def send(key, group, reach):
            return spread(senders[key], 0, wins[key][0], group, pieces(reach, True, key[0] in patched))

        def send_flow(key, group):
            return spread(senders[key], 0, wins[key][0], group, rest if key[0] in patched else flow)

        copies[0].wait()
        p = {z: gl[0, z - base] for z in own_planes}
        v = tuple({z: gl[1 + f, z - base] for z in own_planes} for f in range(3))
        store_wave(senders[("guess", 0)], p, {z: part_div(*v, z) for z in own_planes})
        store_flow(senders[("guess", 0)], v)
        copies[3].wait()

        def gram_step(i, total):
            t = jnp.swapaxes(basis[:, i], 0, 1)
            hi = t.astype(jnp.bfloat16)
            rest = t - hi.astype(jnp.float32)
            mid = rest.astype(jnp.bfloat16)
            low = (rest - mid.astype(jnp.float32)).astype(jnp.bfloat16)
            parts = jnp.concatenate([hi, mid, low], axis=1)
            flat = jnp.concatenate([parts[j] for j in range(parts.shape[0])], axis=1)
            return total + lax.dot_general(
                flat, flat, (((1,), (1,)), ((), ())), preferred_element_type=jnp.float32
            )

        early = 0
        full = lax.fori_loop(0, early, gram_step, jnp.zeros((3 * rank, 3 * rank), jnp.float32))
        copies[1].wait()
        copies[2].wait()
        pl.semaphore_wait(barrier, greetings)

        first = send(("guess", 0), block(2), 4)
        first += spread(fl, 0, fw, block(1), load_pieces(4, True))
        first += spread(cw, base, cw, k, speed_pieces)
        first_flow = send_flow(("guess", 0), block(2))

        full = lax.fori_loop(early, basis.shape[1], gram_step, full)
        hh, hm, hl = full[:rank, :rank], full[:rank, rank:2 * rank], full[:rank, 2 * rank:]
        mh, mm, lh = full[rank:2 * rank, :rank], full[rank:2 * rank, rank:2 * rank], full[2 * rank:, :rank]
        gram = hh + ((hm + mh) + (mm + (hl + lh)))
        gb[s] = jnp.concatenate([gram[:rank // 2], gram[rank // 2:]], axis=1)

        gram_copies = [Remote(gb.at[s], gb.at[s], (k, peer(d))) for d in range(1, n_sp)]

        def narrow_step(r, carry):
            b = [{z: basis[r, f * slab + z - base] for z in own_planes} for f in range(4)]
            for z in own_planes:
                slim[r, z - base] = part_div(*b[1:], z)
                slim[r, slab + z - base] = b[0][z]
            slim[r, 2 * slab] = b[3][base + slab - 1]
            return carry

        lax.fori_loop(0, rank, narrow_step, 0, unroll=2)

        wait(first)
        for z in range(1, 2 * base + slab - 1):
            c2[z] = cw[0, z] * cw[0, z]

        def loads(i, z):
            return fw[i, z]

        p, d = load_window(wins[("guess", 0)][0], 4, True)
        p, d, total = evolve(p, d, 4, DT, loads)
        rel = senders[("relaxed", 0)]
        store_wave(rel, p, d)
        moved = send(("relaxed", 0), block(1), 4)
        wait(first_flow)
        store_flow(rel, push(load_flow(wins[("guess", 0)][0]), total, DT))
        moved_flow = send_flow(("relaxed", 0), block(1))

        def dot(index, p, v):
            for z in own_planes:
                xs[z - base] = p[z]
                for f in range(3):
                    xs[(1 + f) * slab + z - base] = v[f][z]
            x = xs[...]

            def coef_step(i, carry):
                b = basis[pl.ds(8 * i, 8)]
                t = jnp.sum(b * x[None], axis=1)
                half = t.shape[1] // 2
                t = t[:, :half] + t[:, half:]
                acc[pl.ds(pl.multiple_of(8 * i, 8), 8), :] = jnp.sum(t, axis=1)
                return carry

            lax.fori_loop(0, rank // 8, coef_step, 0)
            ones = jnp.ones((8, acc.shape[1]), jnp.float32)
            cf[index, s] = lax.dot_general(
                ones, acc[...], (((1,), (1,)), ((), ())),
                precision=lax.Precision.HIGHEST, preferred_element_type=jnp.float32,
            )
            line = pl.ds(0, 1)
            return [
                Remote(cf.at[index, s, line], cf.at[index, s, line], (k, peer(d)))
                for d in range(1, n_sp)
            ]

        def solve(index, made):
            wait(made)
            total = cf[index, 0, 0:1]
            for i in range(1, n_sp):
                total = total + cf[index, i, 0:1]
            w = jnp.sum(inv[...] * total, axis=1, keepdims=True)
            return jnp.broadcast_to(w, wb.shape)

        def combine(index, made, ref, at):
            wb[...] = solve(index, made)

            def sum_step(r, y):
                return y + wb[pl.ds(r, 1), :][None] * slim[r]

            y = lax.fori_loop(0, rank, sum_step, jnp.zeros(slim.shape[1:], jnp.float32), unroll=8)
            for i in range(slab):
                ref[DV, at + i] = y[i]
                ref[PR, at + i] = y[slab + i]
            ref[VZ, at + slab - 1] = y[2 * slab]

        def coarse(p, d, v):
            h = 4 * DT
            nd = {z: d[z] - h * lap(p, z) for z in own_planes}
            out = {z: p[z] - scale(z, h) * nd[z] for z in own_planes}
            return out, push(v, {z: p[z] for z in range(base, base + slab + 1)}, h), nd

        def corrected(ref, p, v, d):
            q, e = load_window(ref, 4, True)
            h = 4 * DT
            late, ne, total = evolve(q, e, 4, DT)
            change = {z: total[z] - 4.0 * q[z] for z in range(base, base + slab + 1)}
            out, od = {}, {}
            for z in own_planes:
                ce = e[z] - h * lap(q, z)
                out[z] = p[z] + (late[z] - (q[z] - scale(z, h) * ce))
                od[z] = d[z] + (ne[z] - ce)
            return out, push(v, change, DT), od

        wait(gram_copies)
        g = gb[0]
        for i in range(1, n_sp):
            g = g + gb[i]
        g = jnp.concatenate([g, pltpu.roll(g, rank, 1)], axis=0)
        rows = lax.broadcasted_iota(jnp.int32, g.shape, 0)
        lanes = lax.broadcasted_iota(jnp.int32, g.shape, 1)
        m = jnp.where(lanes < rank, g, jnp.where(lanes == rows + rank, 1.0, 0.0))
        def eliminate(m, first, last):
            for j in range(first, last, width):
                part = [jnp.broadcast_to(m[j + i:j + i + 1], (8, m.shape[1])) for i in range(width)]
                e = [[jnp.broadcast_to(r[:, j + i:j + i + 1], r.shape) for i in range(width)] for r in part]
                columns = [m[:, j + i:j + i + 1] for i in range(width)]
                for t in range(width):
                    scaled = 1.0 / e[t][t]
                    part[t] = part[t] * scaled
                    e[t] = [x * scaled for x in e[t]]
                    for i in range(width):
                        if i != t:
                            f = e[i][t]
                            part[i] = part[i] - f * part[t]
                            e[i] = [x - f * y for x, y in zip(e[i], e[t])]
                for i in range(width):
                    m = m - jnp.where((rows >= j) & (rows < j + width), 0.0, columns[i]) * part[i][:1]
                for i in range(width):
                    m = jnp.where(rows == j + i, part[i][:1], m)
            return m

        width = 4 if rank % 4 == 0 else 1
        half = rank // 2 // width * width
        m = eliminate(m, 0, half)
        wait(moved)
        wait(moved_flow)
        p, d = load_window(wins[("relaxed", 0)][0], 4)
        p, d, total = evolve(p, d, 4, DT, loads)
        v = push(load_flow(wins[("relaxed", 0)][0]), total, DT)
        store_wave(tb.at[0], p, d)
        store_flow(tb.at[0], v)
        x = each(minus, (p, v, d), load_state(rel))

        def send_level(i):
            ref = senders[("x", i)]
            store_wave(ref, x[0], x[2])
            store_flow(ref, x[1])
            return send(("x", i), block(1), 1) + send_flow(("x", i), block(1))

        made = dot(0, x[0], x[1])
        x_moved = send_level(0)
        m = eliminate(m, half, rank)
        inverse = m[:, rank:]
        inv[...] = jnp.concatenate([inverse, jnp.zeros_like(inverse)], axis=1)

        res = senders[("x", 0)]
        back = []
        for i in range(3):
            combine(i, made, senders[("y", i)], 0)
            y_moved = send(("y", i), block(1), 4)
            if i == 0:
                back = [Remote(tb.at[0], tb.at[1], (before, s))]
            if i == 1:
                late_loads = spread(fl, 0, fo, k, load_pieces(3, False))
            wait(x_moved)
            ref = wins[("x", i)][0]
            p, d = load_window(ref, 1)
            x = each(plus, coarse(p, d, load_flow(ref)), load_state(res))
            wait(y_moved)
            x = corrected(wins[("y", i)][0], *x)
            if i < 2:
                made = dot(i + 1, x[0], x[1])
                x_moved = send_level(i + 1)

        chains = []
        if n_chain:
            gap = each(minus, x, load_state(senders[("x", 2)]))
            ref = senders[("gap", 1)]
            store_wave(ref, gap[0], gap[2])
            store_flow(ref, gap[1])
        for j in range(1, n_chain + 1):
            chains.append(spread(
                senders[("gap", 1)], 0, wins[("gap", j)][0], block(GROUP * j), pieces(2 * j, True, False) + flow,
                before + GROUP * j < n_tm, before >= GROUP * j,
            ))
        carry = None
        for j in range(n_chain, 0, -1):
            wait(chains[j - 1])
            ref = wins[("gap", j)][0]
            used = before >= GROUP * j
            q, d = load_window(ref, 2 * j)
            u = load_flow(ref)

            def kept(planes):
                return {z: jnp.where(used, planes[z], 0.0) for z in planes}

            q, d, u = kept(q), kept(d), tuple(kept(a) for a in u)
            if carry is not None:
                q = {z: q[z] + carry[0][z] for z in q}
                d = {z: d[z] + carry[1][z] for z in d}
                u = tuple({z: u[f][z] + carry[2][f][z] for z in own_planes} for f in range(3))
            for step in range(2):
                reach = 2 * j - 1 - step
                u = push(u, q, 8 * DT)
                nq, nd = {}, {}
                for z in range(base - reach, base + slab + reach):
                    nd[z] = d[z] - 8 * DT * lap(q, z)
                    nq[z] = q[z] - scale(z, 8 * DT) * nd[z]
                q, d = nq, nd
            carry = (q, d, u)
        if carry is not None:
            x = each(plus, x, (carry[0], carry[2], carry[1]))
        made = dot(3, x[0], x[1])
        ref = wins[("x", 3)][0]
        for z in own_planes:
            ref[PR, z] = x[0][z]
        x_moved = spread(ref, base, ref, k, pieces(1, False, False))
        wait(x_moved)
        wait(back)
        x = each(plus, coarse(load_window(ref, 1)[0], x[2], x[1]), load_state(tb.at[1]))
        ref = wins[("y", 3)][0]
        combine(3, made, ref, base)
        y_moved = spread(ref, base, ref, k, pieces(4, False, True))
        wait(y_moved)
        p, v, d = corrected(ref, *x)
        ref = senders[("final", 0)]
        store_wave(ref, p, d)
        store_flow(ref, v)
        moved = send(("final", 0), block(1), 3) + send_flow(("final", 0), block(1))
        made = dot(4, p, v)
        for z in own_planes:
            states_out[3, 0, z - base] = p[z]
            for f in range(3):
                states_out[3, 1 + f, z - base] = v[f][z]
        w = solve(4, made)
        rows = lax.broadcasted_iota(jnp.int32, w.shape, 0)
        lanes = lax.broadcasted_iota(jnp.int32, w.shape, 1)
        coords_out[...] = jnp.sum(jnp.where(rows == lanes, w, 0.0), axis=0, keepdims=True)[:, :rank]
        wait(late_loads)
        wait(moved)
        p, d = load_window(wins[("final", 0)][0], 3)
        v = load_flow(wins[("final", 0)][0])
        for n in range(3):
            reach = 2 - n
            v = push(v, p, DT)
            fresh, nd = {}, {}
            for z in range(base - reach, base + slab + reach):
                nd[z] = d[z] - DT * lap(p, z)
                source = fl[n, z - base] if z in own_planes else fo[n, z]
                fresh[z] = (p[z] - scale(z, DT) * nd[z]) + source
            p, d = fresh, nd
            for z in own_planes:
                states_out[n, 0, z - base] = p[z]
                for f in range(3):
                    states_out[n, 1 + f, z - base] = v[f][z]
        for c in sent:
            c.wait_send()

    n_wins = 2 + 6 + n_chain + 3
    n_sent = (
        len(pieces(4, True, True)) * 6 + len(pieces(3, True, False)) + len(pieces(1, True, False)) * 4
        + sum(len(pieces(2 * j, True, False)) + 1 for j in range(1, n_chain + 1)) + 7
        + len(load_pieces(4, True)) + len(load_pieces(3, False)) + len(speed_pieces) + 6 * (n_sp - 1) + 1
    )
    return kernel, reach_max, n_wins, n_sent


def solution(mesh):
    n_tm, n_sp = mesh.shape["tm"], mesh.shape["space"]

    def body(speed, forcing, guess, basis):
        rank = basis.shape[1]
        slab, nx, ny = speed.shape
        f32 = jnp.float32
        dma = pltpu.SemaphoreType.DMA
        kernel, reach, n_wins, n_sent = make_kernel(n_tm, n_sp, rank, slab, nx, ny)
        wide = slab + 2 * reach
        return pl.pallas_call(
            kernel,
            out_shape=(
                jax.ShapeDtypeStruct((4, 4, slab, nx, ny), f32),
                jax.ShapeDtypeStruct((1, rank), f32),
            ),
            in_specs=[pl.BlockSpec(memory_space=pltpu.HBM)] * 4,
            out_specs=(pl.BlockSpec(memory_space=pltpu.VMEM),) * 2,
            scratch_shapes=[
                pltpu.VMEM((4, slab, nx, ny), f32),
                pltpu.VMEM((4, slab, nx, ny), f32),
                pltpu.VMEM((rank, 4 * slab, nx, ny), f32),
                pltpu.VMEM((rank, 2 * slab + 1, nx, ny), f32),
                pltpu.VMEM((1, wide, nx, ny), f32),
                pltpu.VMEM((wide, nx, ny), f32),
                pltpu.VMEM((4, wide, nx, ny), f32),
                pltpu.VMEM((3, wide, nx, ny), f32),
                pltpu.VMEM((n_wins, 5, slab, nx, ny), f32),
                pltpu.VMEM((n_wins, 5, wide, nx, ny), f32),
                pltpu.VMEM((4 * slab, nx, ny), f32),
                pltpu.VMEM((2, 5, slab, nx, ny), f32),
                pltpu.VMEM((5, n_sp, 8, 2 * rank), f32),
                pltpu.VMEM((n_sp, rank // 2, 2 * rank), f32),
                pltpu.VMEM((rank, 2 * rank), f32),
                pltpu.VMEM((2 * rank, ny), f32),
                pltpu.VMEM((rank, ny), f32),
                dma((4,)),
                dma((n_sent,)), dma((n_sent,)),
            ],
            compiler_params=pltpu.CompilerParams(
                collective_id=0, has_side_effects=True, vmem_limit_bytes=60 * 1024 * 1024
            ),
        )(speed[None], forcing, guess[0], basis[0].reshape(rank, 4 * slab, nx, ny))

    placed = (
        P("space", None, None),
        P("tm", "space", None, None),
        P("tm", None, "space", None, None),
        P("tm", None, None, "space", None, None),
    )
    return jax.shard_map(
        body,
        mesh=mesh,
        in_specs=placed,
        out_specs=(P("tm", None, "space", None, None), P("tm", None)),
        check_vma=False,
    )
```

```python
import jax
import jax.numpy as jnp
from jax import lax
from jax.experimental import pallas as pl
from jax.experimental.pallas import tpu as pltpu
from jax.sharding import PartitionSpec as P

DT = 0.045
GROUP = 4
MESH = pl.DeviceIdType.MESH
VX, VY, VZ, DV, PR = range(5)


def make_kernel(n_tm, n_sp, rank, slab, nx, ny):
    n_chain = n_tm // GROUP - 1
    reach_max = max(4, 2 * n_chain)
    base = reach_max
    own_planes = range(base, base + slab)

    def span(lo, hi, first):
        lo, hi = max(lo, first), min(hi, first + slab)
        return (lo - first, hi - lo) if hi > lo else None

    def pieces(reach, here, patch):
        made = []
        far = -(-reach // slab)
        for dist in range(far, 0, -1):
            for delta in (dist, -dist):
                first = base - delta * slab
                need = {
                    PR: span(base - reach, base + slab + reach, first),
                    DV: span(base - reach + 1, base + slab + reach - 1, first),
                }
                above = first + slab
                if patch and base - reach + 1 <= above < base + slab + reach - 1:
                    need[VZ] = (slab - 1, 1)
                fields = sorted(need)
                at = 0
                while at < len(fields):
                    end = at + 1
                    while end < len(fields) and need[fields[end]] == need[fields[at]]:
                        end += 1
                    if need[fields[at]] is not None:
                        o, n = need[fields[at]]
                        made.append((delta, fields[at], end - at, o, n))
                    at = end
        if here:
            made.append((0, DV, 2, 0, slab))
            if patch and reach > 1:
                made.append((0, VZ, 1, slab - 1, 1))
        return made

    flow = [(0, VX, 3, 0, slab)]
    rest = [(0, VX, 2, 0, slab)] + ([(0, VZ, 1, 0, slab - 1)] if slab > 1 else [])

    def load_pieces(steps, keep):
        made = []
        far = -(-(steps - 1) // slab)
        for dist in range(far, 0, -1):
            for delta in (dist, -dist):
                first = base - delta * slab
                at = 0
                while at < steps - 1:
                    here = span(base - steps + 1 + at, base + slab + steps - 1 - at, first)
                    end = at + 1
                    while end < steps - 1 and here == span(
                        base - steps + 1 + end, base + slab + steps - 1 - end, first
                    ):
                        end += 1
                    if here is not None:
                        made.append((delta, at, end - at, here[0], here[1]))
                    at = end
        if keep:
            made.append((0, 0, steps, 0, slab))
        return made

    speed_pieces = [(d, 0, 1, o, n) for d, f, m, o, n in pieces(reach_max - 1, False, False) if f <= PR < f + m]

    def kernel(
        speed_in, forcing_in, guess_in, basis_in, states_out, coords_out,
        gl, fl, basis, slim, cw, c2, fw, fo, wv, win, xs, tb, cf, gb, inv, acc, wb,
        local_sem, send_sems, recv_sems,
    ):
        k = lax.axis_index("tm")
        s = lax.axis_index("space")
        before = lax.rem(k + n_tm - 1, n_tm)

        def block(offset):
            return lax.rem(k + offset % n_tm, n_tm)

        def peer(d):
            return lax.rem(s + d, n_sp)

        def inside(at):
            return (at >= 0) & (at < n_sp)


        barrier = pltpu.get_barrier_semaphore()

        def greet(group, at, condition):
            def act():
                pl.semaphore_signal(barrier, inc=1, device_id=(group, at), device_id_type=MESH)

            if condition is None:
                act()
            else:
                pl.when(condition)(act)

        def deltas(reach):
            return sorted({piece[0] for piece in pieces(reach, True, False)}, key=abs)[::-1]

        def one(condition):
            return jnp.where(condition, 1, 0)

        greetings = n_sp
        for off, reach in [(1, 4), (2, 4)]:
            for delta in deltas(reach):
                greet(block(-off), s - delta, None if delta == 0 else inside(s - delta))
                greetings += 1 if delta == 0 else one(inside(s + delta))
        for d in range(n_sp - 1, 0, -1):
            greet(k, peer(d), None)
        for j in range(1, n_chain + 1):
            for delta in deltas(2 * j):
                greet(block(-GROUP * j), s - delta, (before >= GROUP * j) & inside(s - delta))
                greetings += one((before + GROUP * j < n_tm) & inside(s + delta))
        greet(block(1), s, None)

        own = pl.ds(base, slab)
        copies = [
            pltpu.make_async_copy(guess_in, gl, local_sem.at[0]),
            pltpu.make_async_copy(forcing_in, fl, local_sem.at[1]),
            pltpu.make_async_copy(speed_in, cw.at[:, own], local_sem.at[2]),
            pltpu.make_async_copy(basis_in, basis, local_sem.at[3]),
        ]
        for c in copies:
            c.start()

        wins = {}
        senders = {}

        def name(key, reach):
            wins[key] = (win.at[len(wins)], reach)
            senders[key] = wv.at[len(senders)]

        patched = ("guess", "y")
        name(("guess", 0), 4)
        name(("relaxed", 0), 4)
        for i in range(3):
            name(("x", i), 1)
            name(("y", i), 4)
        for j in range(1, n_chain + 1):
            name(("gap", j), 2 * j)
        name(("x", 3), 1)
        name(("y", 3), 4)
        name(("final", 0), 3)

        missing = {}
        for key, (ref, reach) in wins.items():
            for piece in pieces(reach, False, key[0] in patched):
                missing.setdefault(piece[0], []).append((ref, piece))
        for ref, part in ((fw, load_pieces(4, False)), (fo, load_pieces(3, False)), (cw, speed_pieces)):
            for piece in part:
                missing.setdefault(piece[0], []).append((ref, piece))
        for delta, regions in missing.items():
            def clear(regions=regions):
                for ref, (d, f, m, o, n) in regions:
                    at = base - d * slab + o
                    for i in range(f, f + m):
                        ref[i, at:at + n] = jnp.zeros((n, nx, ny), jnp.float32)

            pl.when(jnp.logical_not(inside(s - delta)))(clear)

        sent = []

        class Remote:
            def __init__(self, src, dst, target, sends=None, receives=None):
                i = len(sent)
                self.copy = pltpu.make_async_remote_copy(
                    src_ref=src, dst_ref=dst, send_sem=send_sems.at[i], recv_sem=recv_sems.at[i],
                    device_id=target, device_id_type=MESH,
                )
                self.sends, self.receives = sends, receives
                sent.append(self)
                self.under(sends, self.copy.start)

            def under(self, condition, act):
                if condition is None:
                    act()
                else:
                    pl.when(condition)(act)

            def wait_recv(self):
                self.under(self.receives, self.copy.wait_recv)

            def wait_send(self):
                self.under(self.sends, self.copy.wait_send)

        def both(a, b):
            return b if a is None else a if b is None else a & b

        def spread(src, at, dst, group, parts, sends=None, receives=None):
            made = []
            for delta, f, m, o, n in parts:
                made.append(Remote(
                    src.at[pl.ds(f, m), pl.ds(at + o, n)],
                    dst.at[pl.ds(f, m), pl.ds(base - delta * slab + o, n)],
                    (group, s + delta),
                    both(sends, None if delta == 0 else inside(s + delta)),
                    both(receives, None if delta == 0 else inside(s - delta)),
                ))
            return made

        def wait(made):
            for c in made:
                c.wait_recv()

        row = lax.broadcasted_iota(jnp.int32, (nx, ny), 0)
        lane = lax.broadcasted_iota(jnp.int32, (nx, ny), 1)
        first_row, last_row = row == 0, row == nx - 1
        first_lane, last_lane = lane == 0, lane == ny - 1

        def ahead(p, axis):
            n, last = ((nx, last_row), (ny, last_lane))[axis]
            return jnp.where(last, 0.0, pltpu.roll(p, n - 1, axis))

        def behind(p, axis, border):
            return jnp.where((first_row, first_lane)[axis], border, pltpu.roll(p, 1, axis))

        def floor(z):
            if z <= base and (base - z) % slab == 0:
                return jnp.where(s > (base - z) // slab, 1.0, 0.0)
            return None

        def lap(p, z):
            c = p[z]
            down = c - p[z - 1]
            edge = floor(z)
            if edge is not None:
                down = down * edge
            flat = (ahead(c, 0) + behind(c, 0, c)) + (ahead(c, 1) + behind(c, 1, c)) - 4.0 * c
            return flat + ((p[z + 1] - c) - down)

        def grad(p, z):
            c = p[z]
            return ahead(c, 0) - c, ahead(c, 1) - c, p[z + 1] - c

        def part_div(vx, vy, vz, z):
            d = (vx[z] - behind(vx[z], 0, 0.0)) + (vy[z] - behind(vy[z], 1, 0.0))
            return d + (vz[z] if z == base else vz[z] - vz[z - 1])

        def load_window(ref, reach, patch=False):
            p = {z: ref[PR, z] for z in range(base - reach, base + slab + reach)}
            d = {}
            for z in range(base - reach + 1, base + slab + reach - 1):
                d[z] = ref[DV, z]
                if patch and (z - base) % slab == 0:
                    d[z] = d[z] - ref[VZ, z - 1]
            return p, d

        def load_flow(ref):
            return tuple({z: ref[f, z] for z in own_planes} for f in (VX, VY, VZ))

        def store_wave(ref, p, d):
            for z in own_planes:
                ref[DV, z - base] = d[z]
                ref[PR, z - base] = p[z]

        def store_flow(ref, v):
            for z in own_planes:
                for f in (VX, VY, VZ):
                    ref[f, z - base] = v[f][z]

        def load_state(ref):
            p, d = ({z: ref[f, z - base] for z in own_planes} for f in (PR, DV))
            return p, tuple({z: ref[f, z - base] for z in own_planes} for f in (VX, VY, VZ)), d

        def plus(a, b):
            return {z: a[z] + b[z] for z in own_planes}

        def minus(a, b):
            return {z: a[z] - b[z] for z in own_planes}

        def each(op, a, b):
            return op(a[0], b[0]), tuple(op(x, y) for x, y in zip(a[1], b[1])), op(a[2], b[2])

        def scale(z, h):
            return h * c2[z]

        def evolve(p, d, steps, h, loads=None):
            total = None
            for i in range(steps):
                reach = steps - 1 - i
                kept = {z: p[z] for z in range(base, base + slab + 1)}
                total = kept if total is None else {z: total[z] + kept[z] for z in kept}
                fresh, nd = {}, {}
                for z in range(base - reach, base + slab + reach):
                    nd[z] = d[z] - h * lap(p, z)
                    fresh[z] = p[z] - scale(z, h) * nd[z]
                    if loads is not None:
                        fresh[z] = fresh[z] + loads(i, z)
                p, d = fresh, nd
            return p, d, total

        def push(v, total, h):
            out = ({}, {}, {})
            for z in own_planes:
                g = grad(total, z)
                for f in range(3):
                    out[f][z] = v[f][z] - h * g[f]
            return out

        def send(key, group, reach):
            return spread(senders[key], 0, wins[key][0], group, pieces(reach, True, key[0] in patched))

        def send_flow(key, group):
            return spread(senders[key], 0, wins[key][0], group, rest if key[0] in patched else flow)

        acc[rank:, :] = jnp.zeros((acc.shape[0] - rank, acc.shape[1]), jnp.float32)
        copies[0].wait()
        p = {z: gl[0, z - base] for z in own_planes}
        v = tuple({z: gl[1 + f, z - base] for z in own_planes} for f in range(3))
        store_wave(senders[("guess", 0)], p, {z: part_div(*v, z) for z in own_planes})
        store_flow(senders[("guess", 0)], v)
        copies[3].wait()

        def thirds(t, axis):
            hi = t.astype(jnp.bfloat16)
            rest = t - hi.astype(jnp.float32)
            mid = rest.astype(jnp.bfloat16)
            low = (rest - mid.astype(jnp.float32)).astype(jnp.bfloat16)
            return jnp.concatenate([hi, mid, low], axis=axis)

        def gram_step(i, total):
            t = jnp.swapaxes(basis[:, i], 0, 1)
            parts = thirds(t, 1)
            flat = jnp.concatenate([parts[j] for j in range(parts.shape[0])], axis=1)
            return total + lax.dot_general(
                flat, flat, (((1,), (1,)), ((), ())), preferred_element_type=jnp.float32
            )

        early = 0
        full = lax.fori_loop(0, early, gram_step, jnp.zeros((3 * rank, 3 * rank), jnp.float32))
        copies[1].wait()
        copies[2].wait()
        pl.semaphore_wait(barrier, greetings)

        first = send(("guess", 0), block(2), 4)
        first += spread(fl, 0, fw, block(1), load_pieces(4, True))
        first += spread(cw, base, cw, k, speed_pieces)
        first_flow = send_flow(("guess", 0), block(2))

        full = lax.fori_loop(early, basis.shape[1], gram_step, full)
        hh, hm, hl = full[:rank, :rank], full[:rank, rank:2 * rank], full[:rank, 2 * rank:]
        mh, mm, lh = full[rank:2 * rank, :rank], full[rank:2 * rank, rank:2 * rank], full[2 * rank:, :rank]
        gram = hh + ((hm + mh) + (mm + (hl + lh)))
        gb[s] = jnp.concatenate([gram[:rank // 2], gram[rank // 2:]], axis=1)

        gram_copies = [Remote(gb.at[s], gb.at[s], (k, peer(d))) for d in range(1, n_sp)]

        def narrow_step(r, carry):
            b = [{z: basis[r, f * slab + z - base] for z in own_planes} for f in range(4)]
            for z in own_planes:
                slim[r, z - base] = part_div(*b[1:], z)
                slim[r, slab + z - base] = b[0][z]
            slim[r, 2 * slab] = b[3][base + slab - 1]
            return carry

        lax.fori_loop(0, rank, narrow_step, 0, unroll=2)

        wait(first)
        for z in range(1, 2 * base + slab - 1):
            c2[z] = cw[0, z] * cw[0, z]

        def loads(i, z):
            return fw[i, z]

        p, d = load_window(wins[("guess", 0)][0], 4, True)
        p, d, total = evolve(p, d, 4, DT, loads)
        rel = senders[("relaxed", 0)]
        store_wave(rel, p, d)
        moved = send(("relaxed", 0), block(1), 4)
        wait(first_flow)
        store_flow(rel, push(load_flow(wins[("guess", 0)][0]), total, DT))
        moved_flow = send_flow(("relaxed", 0), block(1))

        def dot(index, p, v):
            for z in own_planes:
                xs[z - base] = p[z]
                for f in range(3):
                    xs[(1 + f) * slab + z - base] = v[f][z]
            x = xs[...]

            def coef_step(i, carry):
                b = basis[pl.ds(8 * i, 8)]
                t = jnp.sum(b * x[None], axis=1)
                half = t.shape[1] // 2
                t = t[:, :half] + t[:, half:]
                acc[pl.ds(pl.multiple_of(8 * i, 8), 8), :] = jnp.sum(t, axis=1)
                return carry

            lax.fori_loop(0, rank // 8, coef_step, 0, unroll=2)
            parts = thirds(acc[...], 1)
            ones = jnp.ones((8, parts.shape[1]), jnp.bfloat16)
            cf[index, s] = lax.dot_general(
                ones, parts, (((1,), (1,)), ((), ())), preferred_element_type=jnp.float32
            )
            line = pl.ds(0, 1)
            return [
                Remote(cf.at[index, s, line], cf.at[index, s, line], (k, peer(d)))
                for d in range(1, n_sp)
            ]

        def solve(index, made):
            wait(made)
            total = cf[index, 0, 0:1]
            for i in range(1, n_sp):
                total = total + cf[index, i, 0:1]
            w = jnp.sum(inv[...] * total, axis=1, keepdims=True)
            return jnp.broadcast_to(w, wb.shape)

        def combine(index, made, ref, at):
            wb[...] = solve(index, made)

            def sum_step(r, y):
                return y + wb[pl.ds(r, 1), :][None] * slim[r]

            y = lax.fori_loop(0, rank, sum_step, jnp.zeros(slim.shape[1:], jnp.float32), unroll=8)
            for i in range(slab):
                ref[DV, at + i] = y[i]
                ref[PR, at + i] = y[slab + i]
            ref[VZ, at + slab - 1] = y[2 * slab]

        def coarse(p, d, v):
            h = 4 * DT
            nd = {z: d[z] - h * lap(p, z) for z in own_planes}
            out = {z: p[z] - scale(z, h) * nd[z] for z in own_planes}
            return out, push(v, {z: p[z] for z in range(base, base + slab + 1)}, h), nd

        def corrected(ref, p, v, d):
            q, e = load_window(ref, 4, True)
            h = 4 * DT
            late, ne, total = evolve(q, e, 4, DT)
            change = {z: total[z] - 4.0 * q[z] for z in range(base, base + slab + 1)}
            out, od = {}, {}
            for z in own_planes:
                ce = e[z] - h * lap(q, z)
                out[z] = p[z] + (late[z] - (q[z] - scale(z, h) * ce))
                od[z] = d[z] + (ne[z] - ce)
            return out, push(v, change, DT), od

        wait(gram_copies)
        g = gb[0]
        for i in range(1, n_sp):
            g = g + gb[i]
        g = jnp.concatenate([g, pltpu.roll(g, rank, 1)], axis=0)
        rows = lax.broadcasted_iota(jnp.int32, g.shape, 0)
        lanes = lax.broadcasted_iota(jnp.int32, g.shape, 1)
        m = jnp.where(lanes < rank, g, jnp.where(lanes == rows + rank, 1.0, 0.0))
        def eliminate(m, first, last):
            for j in range(first, last, width):
                part = [jnp.broadcast_to(m[j + i:j + i + 1], (8, m.shape[1])) for i in range(width)]
                e = [[jnp.broadcast_to(r[:, j + i:j + i + 1], r.shape) for i in range(width)] for r in part]
                columns = [m[:, j + i:j + i + 1] for i in range(width)]
                for t in range(width):
                    scaled = 1.0 / e[t][t]
                    part[t] = part[t] * scaled
                    e[t] = [x * scaled for x in e[t]]
                    for i in range(width):
                        if i != t:
                            f = e[i][t]
                            part[i] = part[i] - f * part[t]
                            e[i] = [x - f * y for x, y in zip(e[i], e[t])]
                for i in range(width):
                    m = m - jnp.where((rows >= j) & (rows < j + width), 0.0, columns[i]) * part[i][:1]
                for i in range(width):
                    m = jnp.where(rows == j + i, part[i][:1], m)
            return m

        width = 8 if rank % 8 == 0 else 1
        half = rank * 3 // 4 // width * width
        m = eliminate(m, 0, half)
        wait(moved)
        wait(moved_flow)
        p, d = load_window(wins[("relaxed", 0)][0], 4)
        p, d, total = evolve(p, d, 4, DT, loads)
        v = push(load_flow(wins[("relaxed", 0)][0]), total, DT)
        store_wave(tb.at[0], p, d)
        store_flow(tb.at[0], v)
        x = each(minus, (p, v, d), load_state(rel))

        def send_level(i):
            ref = senders[("x", i)]
            store_wave(ref, x[0], x[2])
            store_flow(ref, x[1])
            return send(("x", i), block(1), 1) + send_flow(("x", i), block(1))

        made = dot(0, x[0], x[1])
        x_moved = send_level(0)
        m = eliminate(m, half, rank)
        inverse = m[:, rank:]
        inv[...] = jnp.concatenate([inverse, jnp.zeros_like(inverse)], axis=1)

        res = senders[("x", 0)]
        back = []
        for i in range(3):
            combine(i, made, senders[("y", i)], 0)
            y_moved = send(("y", i), block(1), 4)
            if i == 0:
                back = [Remote(tb.at[0], tb.at[1], (before, s))]
            if i == 1:
                late_loads = spread(fl, 0, fo, k, load_pieces(3, False))
            wait(x_moved)
            ref = wins[("x", i)][0]
            p, d = load_window(ref, 1)
            x = each(plus, coarse(p, d, load_flow(ref)), load_state(res))
            wait(y_moved)
            x = corrected(wins[("y", i)][0], *x)
            if i < 2:
                made = dot(i + 1, x[0], x[1])
                x_moved = send_level(i + 1)

        chains = []
        if n_chain:
            gap = each(minus, x, load_state(senders[("x", 2)]))
            ref = senders[("gap", 1)]
            store_wave(ref, gap[0], gap[2])
            store_flow(ref, gap[1])
        for j in range(1, n_chain + 1):
            chains.append(spread(
                senders[("gap", 1)], 0, wins[("gap", j)][0], block(GROUP * j), pieces(2 * j, True, False) + flow,
                before + GROUP * j < n_tm, before >= GROUP * j,
            ))
        carry = None
        for j in range(n_chain, 0, -1):
            wait(chains[j - 1])
            ref = wins[("gap", j)][0]
            used = before >= GROUP * j
            q, d = load_window(ref, 2 * j)
            u = load_flow(ref)

            def kept(planes):
                return {z: jnp.where(used, planes[z], 0.0) for z in planes}

            q, d, u = kept(q), kept(d), tuple(kept(a) for a in u)
            if carry is not None:
                q = {z: q[z] + carry[0][z] for z in q}
                d = {z: d[z] + carry[1][z] for z in d}
                u = tuple({z: u[f][z] + carry[2][f][z] for z in own_planes} for f in range(3))
            for step in range(2):
                reach = 2 * j - 1 - step
                u = push(u, q, 8 * DT)
                nq, nd = {}, {}
                for z in range(base - reach, base + slab + reach):
                    nd[z] = d[z] - 8 * DT * lap(q, z)
                    nq[z] = q[z] - scale(z, 8 * DT) * nd[z]
                q, d = nq, nd
            carry = (q, d, u)
        if carry is not None:
            x = each(plus, x, (carry[0], carry[2], carry[1]))
        made = dot(3, x[0], x[1])
        ref = wins[("x", 3)][0]
        for z in own_planes:
            ref[PR, z] = x[0][z]
        x_moved = spread(ref, base, ref, k, pieces(1, False, False))
        wait(x_moved)
        wait(back)
        x = each(plus, coarse(load_window(ref, 1)[0], x[2], x[1]), load_state(tb.at[1]))
        ref = wins[("y", 3)][0]
        combine(3, made, ref, base)
        y_moved = spread(ref, base, ref, k, pieces(4, False, True))
        wait(y_moved)
        p, v, d = corrected(ref, *x)
        ref = senders[("final", 0)]
        store_wave(ref, p, d)
        store_flow(ref, v)
        moved = send(("final", 0), block(1), 3) + send_flow(("final", 0), block(1))
        made = dot(4, p, v)
        for z in own_planes:
            states_out[3, 0, z - base] = p[z]
            for f in range(3):
                states_out[3, 1 + f, z - base] = v[f][z]
        w = solve(4, made)
        rows = lax.broadcasted_iota(jnp.int32, w.shape, 0)
        lanes = lax.broadcasted_iota(jnp.int32, w.shape, 1)
        coords_out[...] = jnp.sum(jnp.where(rows == lanes, w, 0.0), axis=0, keepdims=True)[:, :rank]
        wait(late_loads)
        wait(moved)
        p, d = load_window(wins[("final", 0)][0], 3)
        v = load_flow(wins[("final", 0)][0])
        for n in range(3):
            reach = 2 - n
            v = push(v, p, DT)
            fresh, nd = {}, {}
            for z in range(base - reach, base + slab + reach):
                nd[z] = d[z] - DT * lap(p, z)
                source = fl[n, z - base] if z in own_planes else fo[n, z]
                fresh[z] = (p[z] - scale(z, DT) * nd[z]) + source
            p, d = fresh, nd
            for z in own_planes:
                states_out[n, 0, z - base] = p[z]
                for f in range(3):
                    states_out[n, 1 + f, z - base] = v[f][z]
        for c in sent:
            c.wait_send()

    n_wins = 2 + 6 + n_chain + 3
    n_sent = (
        len(pieces(4, True, True)) * 6 + len(pieces(3, True, False)) + len(pieces(1, True, False)) * 4
        + sum(len(pieces(2 * j, True, False)) + 1 for j in range(1, n_chain + 1)) + 7
        + len(load_pieces(4, True)) + len(load_pieces(3, False)) + len(speed_pieces) + 6 * (n_sp - 1) + 1
    )
    return kernel, reach_max, n_wins, n_sent


def hand_over(states_in, coords_in, states_out, coords_out):
    states_out[...] = states_in[...]
    coords_out[...] = coords_in[...]


def solution(mesh):
    n_tm, n_sp = mesh.shape["tm"], mesh.shape["space"]

    def body(speed, forcing, guess, basis):
        rank = basis.shape[1]
        slab, nx, ny = speed.shape
        f32 = jnp.float32
        dma = pltpu.SemaphoreType.DMA
        kernel, reach, n_wins, n_sent = make_kernel(n_tm, n_sp, rank, slab, nx, ny)
        wide = slab + 2 * reach
        made = pl.pallas_call(
            kernel,
            out_shape=(
                jax.ShapeDtypeStruct((4, 4, slab, nx, ny), f32),
                jax.ShapeDtypeStruct((1, rank), f32),
            ),
            in_specs=[pl.BlockSpec(memory_space=pltpu.HBM)] * 4,
            out_specs=(pl.BlockSpec(memory_space=pltpu.VMEM),) * 2,
            scratch_shapes=[
                pltpu.VMEM((4, slab, nx, ny), f32),
                pltpu.VMEM((4, slab, nx, ny), f32),
                pltpu.VMEM((rank, 4 * slab, nx, ny), f32),
                pltpu.VMEM((rank, 2 * slab + 1, nx, ny), f32),
                pltpu.VMEM((1, wide, nx, ny), f32),
                pltpu.VMEM((wide, nx, ny), f32),
                pltpu.VMEM((4, wide, nx, ny), f32),
                pltpu.VMEM((3, wide, nx, ny), f32),
                pltpu.VMEM((n_wins, 5, slab, nx, ny), f32),
                pltpu.VMEM((n_wins, 5, wide, nx, ny), f32),
                pltpu.VMEM((4 * slab, nx, ny), f32),
                pltpu.VMEM((2, 5, slab, nx, ny), f32),
                pltpu.VMEM((5, n_sp, 8, 2 * rank), f32),
                pltpu.VMEM((n_sp, rank // 2, 2 * rank), f32),
                pltpu.VMEM((rank, 2 * rank), f32),
                pltpu.VMEM((2 * rank, ny), f32),
                pltpu.VMEM((rank, ny), f32),
                dma((4,)),
                dma((n_sent,)), dma((n_sent,)),
            ],
            compiler_params=pltpu.CompilerParams(
                collective_id=0, has_side_effects=True, vmem_limit_bytes=60 * 1024 * 1024
            ),
        )(speed[None], forcing, guess[0], basis[0].reshape(rank, 4 * slab, nx, ny))
        return pl.pallas_call(
            hand_over,
            out_shape=[jax.ShapeDtypeStruct(a.shape, f32) for a in made],
            in_specs=[pl.BlockSpec(memory_space=pltpu.VMEM)] * 2,
            out_specs=[pl.BlockSpec(memory_space=pltpu.VMEM)] * 2,
        )(*made)

    placed = (
        P("space", None, None),
        P("tm", "space", None, None),
        P("tm", None, "space", None, None),
        P("tm", None, None, "space", None, None),
    )
    return jax.shard_map(
        body,
        mesh=mesh,
        in_specs=placed,
        out_specs=(P("tm", None, "space", None, None), P("tm", None)),
        check_vma=False,
    )
```

```python
import jax
import jax.numpy as jnp
from jax import lax
from jax.experimental import pallas as pl
from jax.experimental.pallas import tpu as pltpu
from jax.sharding import PartitionSpec as P

DT = 0.045
GROUP = 4
MESH = pl.DeviceIdType.MESH
VX, VY, VZ, DV, PR = range(5)


def make_kernel(n_tm, n_sp, rank, slab, nx, ny):
    n_chain = n_tm // GROUP - 1
    reach_max = max(4, 2 * n_chain)
    base = reach_max
    own_planes = range(base, base + slab)

    def span(lo, hi, first):
        lo, hi = max(lo, first), min(hi, first + slab)
        return (lo - first, hi - lo) if hi > lo else None

    def pieces(reach, here, patch):
        made = []
        far = -(-reach // slab)
        for dist in range(far, 0, -1):
            for delta in (dist, -dist):
                first = base - delta * slab
                need = {
                    PR: span(base - reach, base + slab + reach, first),
                    DV: span(base - reach + 1, base + slab + reach - 1, first),
                }
                above = first + slab
                if patch and base - reach + 1 <= above < base + slab + reach - 1:
                    need[VZ] = (slab - 1, 1)
                fields = sorted(need)
                at = 0
                while at < len(fields):
                    end = at + 1
                    while end < len(fields) and need[fields[end]] == need[fields[at]]:
                        end += 1
                    if need[fields[at]] is not None:
                        o, n = need[fields[at]]
                        made.append((delta, fields[at], end - at, o, n))
                    at = end
        if here:
            made.append((0, DV, 2, 0, slab))
            if patch and reach > 1:
                made.append((0, VZ, 1, slab - 1, 1))
        return made

    flow = [(0, VX, 3, 0, slab)]
    rest = [(0, VX, 2, 0, slab)] + ([(0, VZ, 1, 0, slab - 1)] if slab > 1 else [])

    def load_pieces(steps, keep):
        made = []
        far = -(-(steps - 1) // slab)
        for dist in range(far, 0, -1):
            for delta in (dist, -dist):
                first = base - delta * slab
                at = 0
                while at < steps - 1:
                    here = span(base - steps + 1 + at, base + slab + steps - 1 - at, first)
                    end = at + 1
                    while end < steps - 1 and here == span(
                        base - steps + 1 + end, base + slab + steps - 1 - end, first
                    ):
                        end += 1
                    if here is not None:
                        made.append((delta, at, end - at, here[0], here[1]))
                    at = end
        if keep:
            made.append((0, 0, steps, 0, slab))
        return made

    speed_pieces = [(d, 0, 1, o, n) for d, f, m, o, n in pieces(reach_max - 1, False, False) if f <= PR < f + m]

    def kernel(
        speed_in, forcing_in, guess_in, basis_in, states_out, coords_out,
        gl, fl, basis, slim, cw, c2, fw, fo, wv, win, xs, tb, cf, gb, inv, acc, wb,
        local_sem, send_sems, recv_sems,
    ):
        k = lax.axis_index("tm")
        s = lax.axis_index("space")
        before = lax.rem(k + n_tm - 1, n_tm)

        def block(offset):
            return lax.rem(k + offset % n_tm, n_tm)

        def peer(d):
            return lax.rem(s + d, n_sp)

        def inside(at):
            return (at >= 0) & (at < n_sp)


        barrier = pltpu.get_barrier_semaphore()

        def greet(group, at, condition):
            def act():
                pl.semaphore_signal(barrier, inc=1, device_id=(group, at), device_id_type=MESH)

            if condition is None:
                act()
            else:
                pl.when(condition)(act)

        def deltas(reach):
            return sorted({piece[0] for piece in pieces(reach, True, False)}, key=abs)[::-1]

        def one(condition):
            return jnp.where(condition, 1, 0)

        greetings = n_sp
        for off, reach in [(1, 4), (2, 4)]:
            for delta in deltas(reach):
                greet(block(-off), s - delta, None if delta == 0 else inside(s - delta))
                greetings += 1 if delta == 0 else one(inside(s + delta))
        for d in range(n_sp - 1, 0, -1):
            greet(k, peer(d), None)
        for j in range(1, n_chain + 1):
            for delta in deltas(2 * j):
                greet(block(-GROUP * j), s - delta, (before >= GROUP * j) & inside(s - delta))
                greetings += one((before + GROUP * j < n_tm) & inside(s + delta))
        greet(block(1), s, None)

        own = pl.ds(base, slab)
        copies = [
            pltpu.make_async_copy(guess_in, gl, local_sem.at[0]),
            pltpu.make_async_copy(forcing_in, fl, local_sem.at[1]),
            pltpu.make_async_copy(speed_in, cw.at[:, own], local_sem.at[2]),
            pltpu.make_async_copy(basis_in, basis, local_sem.at[3]),
        ]
        for c in copies:
            c.start()

        wins = {}
        senders = {}

        def name(key, reach):
            wins[key] = (win.at[len(wins)], reach)
            senders[key] = wv.at[len(senders)]

        patched = ("guess", "y")
        name(("guess", 0), 4)
        name(("relaxed", 0), 4)
        for i in range(3):
            name(("x", i), 1)
            name(("y", i), 4)
        for j in range(1, n_chain + 1):
            name(("gap", j), 2 * j)
        name(("x", 3), 1)
        name(("y", 3), 4)
        name(("final", 0), 3)

        missing = {}
        for key, (ref, reach) in wins.items():
            for piece in pieces(reach, False, key[0] in patched):
                missing.setdefault(piece[0], []).append((ref, piece))
        for ref, part in ((fw, load_pieces(4, False)), (fo, load_pieces(3, False)), (cw, speed_pieces)):
            for piece in part:
                missing.setdefault(piece[0], []).append((ref, piece))
        for delta, regions in missing.items():
            def clear(regions=regions):
                for ref, (d, f, m, o, n) in regions:
                    at = base - d * slab + o
                    for i in range(f, f + m):
                        ref[i, at:at + n] = jnp.zeros((n, nx, ny), jnp.float32)

            pl.when(jnp.logical_not(inside(s - delta)))(clear)

        sent = []

        class Remote:
            def __init__(self, src, dst, target, sends=None, receives=None):
                i = len(sent)
                self.copy = pltpu.make_async_remote_copy(
                    src_ref=src, dst_ref=dst, send_sem=send_sems.at[i], recv_sem=recv_sems.at[i],
                    device_id=target, device_id_type=MESH,
                )
                self.sends, self.receives = sends, receives
                sent.append(self)
                self.under(sends, self.copy.start)

            def under(self, condition, act):
                if condition is None:
                    act()
                else:
                    pl.when(condition)(act)

            def wait_recv(self):
                self.under(self.receives, self.copy.wait_recv)

            def wait_send(self):
                self.under(self.sends, self.copy.wait_send)

        def both(a, b):
            return b if a is None else a if b is None else a & b

        def spread(src, at, dst, group, parts, sends=None, receives=None):
            made = []
            for delta, f, m, o, n in parts:
                made.append(Remote(
                    src.at[pl.ds(f, m), pl.ds(at + o, n)],
                    dst.at[pl.ds(f, m), pl.ds(base - delta * slab + o, n)],
                    (group, s + delta),
                    both(sends, None if delta == 0 else inside(s + delta)),
                    both(receives, None if delta == 0 else inside(s - delta)),
                ))
            return made

        def wait(made):
            for c in made:
                c.wait_recv()

        row = lax.broadcasted_iota(jnp.int32, (nx, ny), 0)
        lane = lax.broadcasted_iota(jnp.int32, (nx, ny), 1)
        first_row, last_row = row == 0, row == nx - 1
        first_lane, last_lane = lane == 0, lane == ny - 1

        def ahead(p, axis):
            n, last = ((nx, last_row), (ny, last_lane))[axis]
            return jnp.where(last, 0.0, pltpu.roll(p, n - 1, axis))

        def behind(p, axis, border):
            return jnp.where((first_row, first_lane)[axis], border, pltpu.roll(p, 1, axis))

        def floor(z):
            if z <= base and (base - z) % slab == 0:
                return jnp.where(s > (base - z) // slab, 1.0, 0.0)
            return None

        def lap(p, z):
            c = p[z]
            down = c - p[z - 1]
            edge = floor(z)
            if edge is not None:
                down = down * edge
            flat = (ahead(c, 0) + behind(c, 0, c)) + (ahead(c, 1) + behind(c, 1, c)) - 4.0 * c
            return flat + ((p[z + 1] - c) - down)

        def grad(p, z):
            c = p[z]
            return ahead(c, 0) - c, ahead(c, 1) - c, p[z + 1] - c

        def part_div(vx, vy, vz, z):
            d = (vx[z] - behind(vx[z], 0, 0.0)) + (vy[z] - behind(vy[z], 1, 0.0))
            return d + (vz[z] if z == base else vz[z] - vz[z - 1])

        def load_window(ref, reach, patch=False):
            p = {z: ref[PR, z] for z in range(base - reach, base + slab + reach)}
            d = {}
            for z in range(base - reach + 1, base + slab + reach - 1):
                d[z] = ref[DV, z]
                if patch and (z - base) % slab == 0:
                    d[z] = d[z] - ref[VZ, z - 1]
            return p, d

        def load_flow(ref):
            return tuple({z: ref[f, z] for z in own_planes} for f in (VX, VY, VZ))

        def store_wave(ref, p, d):
            for z in own_planes:
                ref[DV, z - base] = d[z]
                ref[PR, z - base] = p[z]

        def store_flow(ref, v):
            for z in own_planes:
                for f in (VX, VY, VZ):
                    ref[f, z - base] = v[f][z]

        def load_state(ref):
            p, d = ({z: ref[f, z - base] for z in own_planes} for f in (PR, DV))
            return p, tuple({z: ref[f, z - base] for z in own_planes} for f in (VX, VY, VZ)), d

        def plus(a, b):
            return {z: a[z] + b[z] for z in own_planes}

        def minus(a, b):
            return {z: a[z] - b[z] for z in own_planes}

        def each(op, a, b):
            return op(a[0], b[0]), tuple(op(x, y) for x, y in zip(a[1], b[1])), op(a[2], b[2])

        def scale(z, h):
            return h * c2[z]

        def evolve(p, d, steps, h, loads=None):
            total = None
            for i in range(steps):
                reach = steps - 1 - i
                kept = {z: p[z] for z in range(base, base + slab + 1)}
                total = kept if total is None else {z: total[z] + kept[z] for z in kept}
                fresh, nd = {}, {}
                for z in range(base - reach, base + slab + reach):
                    nd[z] = d[z] - h * lap(p, z)
                    fresh[z] = p[z] - scale(z, h) * nd[z]
                    if loads is not None:
                        fresh[z] = fresh[z] + loads(i, z)
                p, d = fresh, nd
            return p, d, total

        def push(v, total, h):
            out = ({}, {}, {})
            for z in own_planes:
                g = grad(total, z)
                for f in range(3):
                    out[f][z] = v[f][z] - h * g[f]
            return out

        def send(key, group, reach):
            return spread(senders[key], 0, wins[key][0], group, pieces(reach, True, key[0] in patched))

        def send_flow(key, group):
            return spread(senders[key], 0, wins[key][0], group, rest if key[0] in patched else flow)

        acc[rank:, :] = jnp.zeros((acc.shape[0] - rank, acc.shape[1]), jnp.float32)
        copies[0].wait()
        p = {z: gl[0, z - base] for z in own_planes}
        v = tuple({z: gl[1 + f, z - base] for z in own_planes} for f in range(3))
        store_wave(senders[("guess", 0)], p, {z: part_div(*v, z) for z in own_planes})
        store_flow(senders[("guess", 0)], v)
        copies[3].wait()

        def thirds(t, axis):
            hi = t.astype(jnp.bfloat16)
            rest = t - hi.astype(jnp.float32)
            mid = rest.astype(jnp.bfloat16)
            low = (rest - mid.astype(jnp.float32)).astype(jnp.bfloat16)
            return jnp.concatenate([hi, mid, low], axis=axis)

        def gram_step(i, total):
            t = jnp.swapaxes(basis[:, i], 0, 1)
            parts = thirds(t, 1)
            flat = jnp.concatenate([parts[j] for j in range(parts.shape[0])], axis=1)
            return total + lax.dot_general(
                flat, flat, (((1,), (1,)), ((), ())), preferred_element_type=jnp.float32
            )

        early = 0
        full = lax.fori_loop(0, early, gram_step, jnp.zeros((3 * rank, 3 * rank), jnp.float32))
        copies[1].wait()
        copies[2].wait()
        pl.semaphore_wait(barrier, greetings)

        first = send(("guess", 0), block(2), 4)
        first += spread(fl, 0, fw, block(1), load_pieces(4, True))
        first += spread(cw, base, cw, k, speed_pieces)
        first_flow = send_flow(("guess", 0), block(2))

        full = lax.fori_loop(early, basis.shape[1], gram_step, full)
        hh, hm, hl = full[:rank, :rank], full[:rank, rank:2 * rank], full[:rank, 2 * rank:]
        mh, mm, lh = full[rank:2 * rank, :rank], full[rank:2 * rank, rank:2 * rank], full[2 * rank:, :rank]
        gram = hh + ((hm + mh) + (mm + (hl + lh)))
        gb[s] = jnp.concatenate([gram[:rank // 2], gram[rank // 2:]], axis=1)

        gram_copies = [Remote(gb.at[s], gb.at[s], (k, peer(d))) for d in range(1, n_sp)]

        def narrow_step(r, carry):
            b = [{z: basis[r, f * slab + z - base] for z in own_planes} for f in range(4)]
            for z in own_planes:
                slim[r, z - base] = part_div(*b[1:], z)
                slim[r, slab + z - base] = b[0][z]
            slim[r, 2 * slab] = b[3][base + slab - 1]
            return carry

        lax.fori_loop(0, rank, narrow_step, 0, unroll=2)

        wait(first)
        for z in range(1, 2 * base + slab - 1):
            c2[z] = cw[0, z] * cw[0, z]

        def loads(i, z):
            return fw[i, z]

        p, d = load_window(wins[("guess", 0)][0], 4, True)
        p, d, total = evolve(p, d, 4, DT, loads)
        rel = senders[("relaxed", 0)]
        store_wave(rel, p, d)
        moved = send(("relaxed", 0), block(1), 4)
        wait(first_flow)
        store_flow(rel, push(load_flow(wins[("guess", 0)][0]), total, DT))
        moved_flow = send_flow(("relaxed", 0), block(1))

        def dot(index, p, v):
            for z in own_planes:
                xs[z - base] = p[z]
                for f in range(3):
                    xs[(1 + f) * slab + z - base] = v[f][z]
            x = xs[...]

            def coef_step(i, carry):
                b = basis[pl.ds(8 * i, 8)]
                t = jnp.sum(b * x[None], axis=1)
                half = t.shape[1] // 2
                t = t[:, :half] + t[:, half:]
                acc[pl.ds(pl.multiple_of(8 * i, 8), 8), :] = jnp.sum(t, axis=1)
                return carry

            lax.fori_loop(0, rank // 8, coef_step, 0, unroll=2)
            parts = thirds(acc[...], 1)
            ones = jnp.ones((8, parts.shape[1]), jnp.bfloat16)
            cf[index, s] = lax.dot_general(
                ones, parts, (((1,), (1,)), ((), ())), preferred_element_type=jnp.float32
            )
            line = pl.ds(0, 1)
            return [
                Remote(cf.at[index, s, line], cf.at[index, s, line], (k, peer(d)))
                for d in range(1, n_sp)
            ]

        def solve(index, made):
            wait(made)
            total = cf[index, 0, 0:1]
            for i in range(1, n_sp):
                total = total + cf[index, i, 0:1]
            w = jnp.sum(inv[...] * total, axis=1, keepdims=True)
            return jnp.broadcast_to(w, wb.shape)

        def combine(index, made, ref, at):
            wb[...] = solve(index, made)

            def sum_step(r, y):
                return y + wb[pl.ds(r, 1), :][None] * slim[r]

            y = lax.fori_loop(0, rank, sum_step, jnp.zeros(slim.shape[1:], jnp.float32), unroll=8)
            for i in range(slab):
                ref[DV, at + i] = y[i]
                ref[PR, at + i] = y[slab + i]
            ref[VZ, at + slab - 1] = y[2 * slab]

        def coarse(p, d, v):
            h = 4 * DT
            nd = {z: d[z] - h * lap(p, z) for z in own_planes}
            out = {z: p[z] - scale(z, h) * nd[z] for z in own_planes}
            return out, push(v, {z: p[z] for z in range(base, base + slab + 1)}, h), nd

        def corrected(ref, p, v, d):
            q, e = load_window(ref, 4, True)
            h = 4 * DT
            late, ne, total = evolve(q, e, 4, DT)
            change = {z: total[z] - 4.0 * q[z] for z in range(base, base + slab + 1)}
            out, od = {}, {}
            for z in own_planes:
                ce = e[z] - h * lap(q, z)
                out[z] = p[z] + (late[z] - (q[z] - scale(z, h) * ce))
                od[z] = d[z] + (ne[z] - ce)
            return out, push(v, change, DT), od

        wait(gram_copies)
        g = gb[0]
        for i in range(1, n_sp):
            g = g + gb[i]
        g = jnp.concatenate([g, pltpu.roll(g, rank, 1)], axis=0)
        rows = lax.broadcasted_iota(jnp.int32, g.shape, 0)
        lanes = lax.broadcasted_iota(jnp.int32, g.shape, 1)
        m = jnp.where(lanes < rank, g, jnp.where(lanes == rows + rank, 1.0, 0.0))
        def eliminate(m, first, last):
            for j in range(first, last, width):
                part = [jnp.broadcast_to(m[j + i:j + i + 1], (8, m.shape[1])) for i in range(width)]
                e = [[jnp.broadcast_to(r[:, j + i:j + i + 1], r.shape) for i in range(width)] for r in part]
                columns = [m[:, j + i:j + i + 1] for i in range(width)]
                for t in range(width):
                    scaled = 1.0 / e[t][t]
                    part[t] = part[t] * scaled
                    e[t] = [x * scaled for x in e[t]]
                    for i in range(width):
                        if i != t:
                            f = e[i][t]
                            part[i] = part[i] - f * part[t]
                            e[i] = [x - f * y for x, y in zip(e[i], e[t])]
                for i in range(width):
                    m = m - jnp.where((rows >= j) & (rows < j + width), 0.0, columns[i]) * part[i][:1]
                for i in range(width):
                    m = jnp.where(rows == j + i, part[i][:1], m)
            return m

        width = 8 if rank % 8 == 0 else 1
        half = rank * 3 // 4 // width * width
        m = eliminate(m, 0, half)
        wait(moved)
        p, d = load_window(wins[("relaxed", 0)][0], 4)
        p, d, total = evolve(p, d, 4, DT, loads)
        store_wave(tb.at[0], p, d)
        wait(moved_flow)
        v = push(load_flow(wins[("relaxed", 0)][0]), total, DT)
        store_flow(tb.at[0], v)
        x = each(minus, (p, v, d), load_state(rel))

        def send_level(i):
            ref = senders[("x", i)]
            store_wave(ref, x[0], x[2])
            store_flow(ref, x[1])
            return send(("x", i), block(1), 1) + send_flow(("x", i), block(1))

        made = dot(0, x[0], x[1])
        x_moved = send_level(0)
        m = eliminate(m, half, rank)
        inverse = m[:, rank:]
        inv[...] = jnp.concatenate([inverse, jnp.zeros_like(inverse)], axis=1)

        res = senders[("x", 0)]
        back = []
        for i in range(3):
            combine(i, made, senders[("y", i)], 0)
            y_moved = send(("y", i), block(1), 4)
            if i == 0:
                back = [Remote(tb.at[0], tb.at[1], (before, s))]
            if i == 1:
                late_loads = spread(fl, 0, fo, k, load_pieces(3, False))
            wait(x_moved)
            ref = wins[("x", i)][0]
            p, d = load_window(ref, 1)
            x = each(plus, coarse(p, d, load_flow(ref)), load_state(res))
            wait(y_moved)
            x = corrected(wins[("y", i)][0], *x)
            if i < 2:
                made = dot(i + 1, x[0], x[1])
                x_moved = send_level(i + 1)

        chains = []
        if n_chain:
            gap = each(minus, x, load_state(senders[("x", 2)]))
            ref = senders[("gap", 1)]
            store_wave(ref, gap[0], gap[2])
            store_flow(ref, gap[1])
        for j in range(1, n_chain + 1):
            chains.append(spread(
                senders[("gap", 1)], 0, wins[("gap", j)][0], block(GROUP * j), pieces(2 * j, True, False) + flow,
                before + GROUP * j < n_tm, before >= GROUP * j,
            ))
        carry = None
        for j in range(n_chain, 0, -1):
            wait(chains[j - 1][:-1])
            ref = wins[("gap", j)][0]
            used = before >= GROUP * j
            q, d = load_window(ref, 2 * j)

            def kept(planes):
                return {z: jnp.where(used, planes[z], 0.0) for z in planes}

            q, d = kept(q), kept(d)
            if carry is not None:
                q = {z: q[z] + carry[0][z] for z in q}
                d = {z: d[z] + carry[1][z] for z in d}
            before_steps = []
            for step in range(2):
                reach = 2 * j - 1 - step
                before_steps.append(q)
                nq, nd = {}, {}
                for z in range(base - reach, base + slab + reach):
                    nd[z] = d[z] - 8 * DT * lap(q, z)
                    nq[z] = q[z] - scale(z, 8 * DT) * nd[z]
                q, d = nq, nd
            wait(chains[j - 1][-1:])
            u = tuple(kept(a) for a in load_flow(ref))
            if carry is not None:
                u = tuple({z: u[f][z] + carry[2][f][z] for z in own_planes} for f in range(3))
            for planes in before_steps:
                u = push(u, planes, 8 * DT)
            carry = (q, d, u)
        if carry is not None:
            x = each(plus, x, (carry[0], carry[2], carry[1]))
        made = dot(3, x[0], x[1])
        ref = wins[("x", 3)][0]
        for z in own_planes:
            ref[PR, z] = x[0][z]
        x_moved = spread(ref, base, ref, k, pieces(1, False, False))
        wait(x_moved)
        wait(back)
        x = each(plus, coarse(load_window(ref, 1)[0], x[2], x[1]), load_state(tb.at[1]))
        ref = wins[("y", 3)][0]
        combine(3, made, ref, base)
        y_moved = spread(ref, base, ref, k, pieces(4, False, True))
        wait(y_moved)
        p, v, d = corrected(ref, *x)
        ref = senders[("final", 0)]
        store_wave(ref, p, d)
        store_flow(ref, v)
        moved = send(("final", 0), block(1), 3) + send_flow(("final", 0), block(1))
        made = dot(4, p, v)
        for z in own_planes:
            states_out[3, 0, z - base] = p[z]
            for f in range(3):
                states_out[3, 1 + f, z - base] = v[f][z]
        w = solve(4, made)
        rows = lax.broadcasted_iota(jnp.int32, w.shape, 0)
        lanes = lax.broadcasted_iota(jnp.int32, w.shape, 1)
        coords_out[...] = jnp.sum(jnp.where(rows == lanes, w, 0.0), axis=0, keepdims=True)[:, :rank]
        wait(late_loads)
        wait(moved)
        p, d = load_window(wins[("final", 0)][0], 3)
        v = load_flow(wins[("final", 0)][0])
        for n in range(3):
            reach = 2 - n
            v = push(v, p, DT)
            fresh, nd = {}, {}
            for z in range(base - reach, base + slab + reach):
                nd[z] = d[z] - DT * lap(p, z)
                source = fl[n, z - base] if z in own_planes else fo[n, z]
                fresh[z] = (p[z] - scale(z, DT) * nd[z]) + source
            p, d = fresh, nd
            for z in own_planes:
                states_out[n, 0, z - base] = p[z]
                for f in range(3):
                    states_out[n, 1 + f, z - base] = v[f][z]
        for c in sent:
            c.wait_send()

    n_wins = 2 + 6 + n_chain + 3
    n_sent = (
        len(pieces(4, True, True)) * 6 + len(pieces(3, True, False)) + len(pieces(1, True, False)) * 4
        + sum(len(pieces(2 * j, True, False)) + 1 for j in range(1, n_chain + 1)) + 7
        + len(load_pieces(4, True)) + len(load_pieces(3, False)) + len(speed_pieces) + 6 * (n_sp - 1) + 1
    )
    return kernel, reach_max, n_wins, n_sent


def hand_over(states_in, coords_in, states_out, coords_out):
    states_out[...] = states_in[...]
    coords_out[...] = coords_in[...]


def solution(mesh):
    n_tm, n_sp = mesh.shape["tm"], mesh.shape["space"]

    def body(speed, forcing, guess, basis):
        rank = basis.shape[1]
        slab, nx, ny = speed.shape
        f32 = jnp.float32
        dma = pltpu.SemaphoreType.DMA
        kernel, reach, n_wins, n_sent = make_kernel(n_tm, n_sp, rank, slab, nx, ny)
        wide = slab + 2 * reach
        made = pl.pallas_call(
            kernel,
            out_shape=(
                jax.ShapeDtypeStruct((4, 4, slab, nx, ny), f32),
                jax.ShapeDtypeStruct((1, rank), f32),
            ),
            in_specs=[pl.BlockSpec(memory_space=pltpu.HBM)] * 4,
            out_specs=(pl.BlockSpec(memory_space=pltpu.VMEM),) * 2,
            scratch_shapes=[
                pltpu.VMEM((4, slab, nx, ny), f32),
                pltpu.VMEM((4, slab, nx, ny), f32),
                pltpu.VMEM((rank, 4 * slab, nx, ny), f32),
                pltpu.VMEM((rank, 2 * slab + 1, nx, ny), f32),
                pltpu.VMEM((1, wide, nx, ny), f32),
                pltpu.VMEM((wide, nx, ny), f32),
                pltpu.VMEM((4, wide, nx, ny), f32),
                pltpu.VMEM((3, wide, nx, ny), f32),
                pltpu.VMEM((n_wins, 5, slab, nx, ny), f32),
                pltpu.VMEM((n_wins, 5, wide, nx, ny), f32),
                pltpu.VMEM((4 * slab, nx, ny), f32),
                pltpu.VMEM((2, 5, slab, nx, ny), f32),
                pltpu.VMEM((5, n_sp, 8, 2 * rank), f32),
                pltpu.VMEM((n_sp, rank // 2, 2 * rank), f32),
                pltpu.VMEM((rank, 2 * rank), f32),
                pltpu.VMEM((2 * rank, ny), f32),
                pltpu.VMEM((rank, ny), f32),
                dma((4,)),
                dma((n_sent,)), dma((n_sent,)),
            ],
            compiler_params=pltpu.CompilerParams(
                collective_id=0, has_side_effects=True, vmem_limit_bytes=60 * 1024 * 1024
            ),
        )(speed[None], forcing, guess[0], basis[0].reshape(rank, 4 * slab, nx, ny))
        return pl.pallas_call(
            hand_over,
            out_shape=[jax.ShapeDtypeStruct(a.shape, f32) for a in made],
            in_specs=[pl.BlockSpec(memory_space=pltpu.VMEM)] * 2,
            out_specs=[pl.BlockSpec(memory_space=pltpu.VMEM)] * 2,
        )(*made)

    placed = (
        P("space", None, None),
        P("tm", "space", None, None),
        P("tm", None, "space", None, None),
        P("tm", None, None, "space", None, None),
    )
    return jax.shard_map(
        body,
        mesh=mesh,
        in_specs=placed,
        out_specs=(P("tm", None, "space", None, None), P("tm", None)),
        check_vma=False,
    )
```
